256 devices in a mesh: seq: 16 (over z, core), vocab: 16 (over y, x).
Axes of the slice: x: 4, y: 4, z: 8, core: 2. Of those that a mesh axis runs over, the one named last changes fastest.
Arguments:
- probe_states: bfloat16 [3, 16384, 6144], P(None, 'seq', 'vocab'), may hold values from -6 to 6
- final_states: bfloat16 [16384, 6144], P('seq', 'vocab'), may hold values from -6 to 6
- translator: bfloat16 [3, 6144, 6144], P(None, 'vocab', 'seq'), may hold values from -0.078125 to 0.078125
- translator_bias: float32 [3, 6144], P(None, 'seq'), may hold values from -4 to 4
- norm_gain: float32 [6144], P('seq'), may hold values from 0.5 to 1.5
- unembed: bfloat16 [32768, 6144], P('vocab', 'seq'), may hold values from -0.21875 to 0.21875
- answer_rows: int32 [16, 32], P('seq'), may hold values from 0 to 1023, as said below
- answer_count: int32 [16], P('seq'), may hold values from 1 to 32, 256 in all
- targets: int32 [16, 32], P('seq'), may hold values from 0 to 32767
Outputs:
- answer_logprob: float32 [4, 16, 32], P(None, 'seq')
- answer_kl: float32 [3, 16, 32], P(None, 'seq')
The draws below stay inside these ranges and needn't reach their ends.
Inputs may be any that keep to these rules, and one draw needn't show every extreme that they name: `answer_rows`: each row holds 32 different positions. `answer_count`: the counts sum to 256, and some sequence has 32.
All inputs are finite; a program needn't handle non-finite values. No bound on the sum of `answer_count` on one device may be relied on, other than what follows from the above.
Results may differ from the reference program's by a relative error of at most 0.00099.
Values may be sent and summed in bfloat16 or wider, within the bound.
No kernel may reach another device: no remote copies, remote signals or barrier semaphores. Data moves between devices by JAX's collectives and lax.ppermute only.
A program may use at most 64 MiB of HBM per device.

```python
import math
import jax
import jax.numpy as jnp
import numpy as np
from jax import lax

D = 6144
V = 32768
LAYERS = 3
LENGTH = 1024
CAP = 32
SEQS = 16
TOKENS = 16384
FLAGGED = 256


def draw_answer_rows(key, part):
    seqs = TOKENS // LENGTH
    scores = jax.random.randint(key, (seqs, LENGTH), 0, 1 << 20)
    scores = scores * LENGTH + jnp.arange(LENGTH, dtype=jnp.int32)[None, :]
    order = jnp.argsort(scores, axis=1)
    return order[:, :CAP].astype(jnp.int32)


def place_ends(drawn, stream_key, least, high):
    spot = [jax.random.randint(jax.random.fold_in(stream_key, axis), (), 0, length) for axis, length in enumerate(drawn.shape)]
    widest = drawn.shape.index(max(drawn.shape))
    neighbour = spot[:widest] + [(spot[widest] + 1) % drawn.shape[widest]] + spot[widest + 1:]
    return drawn.at[tuple(spot)].set(least).at[tuple(neighbour)].set(high)


def block_scale(key, extent, shards, least, largest):
    def one(dim, blocks):
        heights = jax.random.uniform(jax.random.fold_in(jax.random.fold_in(key, 6), dim), (blocks,), jnp.float32, least / len(shards), largest / len(shards))
        return jnp.repeat(jnp.exp(heights), extent[dim] // blocks).reshape((-1,) + (1,) * (len(extent) - dim - 1))

    gain = one(*shards[0])
    for cut in shards[1:]:
        gain = gain * one(*cut)
    return gain


def rank_table(number_of, lean):
    weights = [(1 << 20) // math.isqrt(standing ** lean) + 1 for standing in range(1, number_of + 1)]
    scale = 1 + sum(weights) // (1 << 30)
    return np.cumsum(np.array([max(1, weight // scale) for weight in weights]))


def ranked(stream_key, extent, number_of, lean):
    grid = rank_table(number_of, lean)
    ticket = jax.random.randint(jax.random.fold_in(stream_key, 1), extent, 0, int(grid[number_of - 1]))
    rank = jnp.searchsorted(jnp.asarray(grid, jnp.int32), ticket, side="right")
    return jax.random.permutation(jax.random.fold_in(stream_key, 2), number_of)[rank].astype(jnp.int32)


def length_profile(count, total, bound, skew):
    weights = [(1 << 20) // math.isqrt(rank ** skew) + 1 for rank in range(2, count + 1)]
    rest, counts = total - bound - (count - 1), [1] * (count - 1)
    while rest > 0:
        free = [i for i in range(count - 1) if counts[i] < bound]
        mass, budget = sum([weights[i] for i in free]), rest
        for i in free:
            extra = min(bound - counts[i], max(1, budget * weights[i] // mass), rest)
            counts[i] = counts[i] + extra
            rest = rest - extra
    return np.array([bound] + counts)


def ragged_sizes(key, amount, total, most, lean):
    if amount == 2:
        one = jax.random.randint(key, (), max(1, total - most), min(most, total - 1) + 1)
        return jnp.stack([one, total - one])
    tallies = jnp.asarray(length_profile(amount, total, most, lean), jnp.int32)
    twos = (amount - 1) // 2
    giver, receiver = tallies[1:1 + 2 * twos:2], tallies[2:2 + 2 * twos:2]
    room = jnp.minimum(giver - 1, most - receiver)
    shifted = jax.random.randint(jax.random.fold_in(key, 1), (twos,), 0, 1 << 20) % (room + 1)
    tallies = tallies.at[1:1 + 2 * twos:2].set(giver - shifted).at[2:2 + 2 * twos:2].set(receiver + shifted)
    return tallies[jax.random.permutation(jax.random.fold_in(key, 2), amount)]


def gaussian(own_key, dims, deviation, reach, split=(), kind=jnp.bfloat16):
    result = deviation * jax.random.normal(own_key, dims, jnp.float32)
    if split:
        result = result * block_scale(own_key, dims, split, -0.22, 0.18)
    return jnp.clip(result, -reach, reach).astype(kind)


def setup_inputs(seed: int = 0) -> dict:
    key_of = jax.random.split(jax.random.key(seed), 10)
    probe_states = gaussian(key_of[0], (LAYERS, TOKENS, D), 1.0, 6.0, ((1, 16), (2, 16)))
    final_states = gaussian(key_of[1], (TOKENS, D), 1.0, 6.0, ((0, 16), (1, 16)))
    translator = gaussian(key_of[2], (LAYERS, D, D), D ** -0.5, 0.078125, ((1, 16), (2, 16)))
    translator_bias = gaussian(key_of[3], (LAYERS, D), 0.5, 4.0, ((1, 16),), jnp.float32)
    norm_gain = jnp.clip(1.0 + 0.1 * jax.random.normal(key_of[4], (D,), jnp.float32), 0.5, 1.5)
    unembed = gaussian(key_of[5], (V, D), (D // 9) ** -0.5, 0.21875, ((0, 16), (1, 16)))
    answer_rows = draw_answer_rows(jax.random.fold_in(key_of[9], 71), 0)
    answer_count = ragged_sizes(key_of[7], SEQS, FLAGGED, CAP, 2).astype(jnp.int32)
    targets = place_ends(ranked(key_of[8], (SEQS, CAP), V, 2), jax.random.fold_in(key_of[8], 3), 0, V - 1).astype(jnp.int32)
    return {"probe_states": probe_states, "final_states": final_states, "translator": translator, "translator_bias": translator_bias, "norm_gain": norm_gain, "unembed": unembed, "answer_rows": answer_rows, "answer_count": answer_count, "targets": targets}


def lens_logits(rows, norm_gain, unembed_f):
    mean_sq = lax.optimization_barrier(jnp.mean(rows * rows, axis=-1))
    scaled = (rows * norm_gain).astype(jnp.bfloat16)
    raw = jnp.dot(scaled.astype(jnp.float32), unembed_f.T, precision=lax.Precision.HIGHEST)
    return raw * lax.rsqrt(mean_sq + 1e-05)[:, None]

def reference(probe_states, final_states, translator, translator_bias, norm_gain, unembed, answer_rows, answer_count, targets):
    seqs = answer_rows.shape[0]
    flat = (jnp.arange(seqs, dtype=jnp.int32)[:, None] * LENGTH + answer_rows.astype(jnp.int32)).reshape(-1)
    live = (jnp.arange(CAP, dtype=jnp.int32)[None, :] < answer_count[:, None]).reshape(-1)
    wanted = targets.reshape(-1)[:, None]
    unembed_f = unembed.astype(jnp.float32)
    final_rows = jnp.take(final_states, flat, axis=0).astype(jnp.float32)
    final_logits = lens_logits(final_rows, norm_gain, unembed_f)
    final_lse = jnp.log(lax.optimization_barrier(jnp.sum(jnp.exp(final_logits), axis=-1)))
    final_prob = jnp.exp(final_logits - final_lse[:, None])
    logprobs = []
    divergences = []
    for layer in range(LAYERS):
        rows = jnp.take(probe_states[layer], flat, axis=0)
        lensed = rows.astype(jnp.float32) + jnp.dot(rows.astype(jnp.float32), translator[layer].astype(jnp.float32), precision=lax.Precision.HIGHEST) + translator_bias[layer]
        logits = lens_logits(lensed, norm_gain, unembed_f)
        lse = jnp.log(lax.optimization_barrier(jnp.sum(jnp.exp(logits), axis=-1)))
        logprobs.append(jnp.take_along_axis(logits, wanted, axis=1)[:, 0] - lse)
        divergences.append(lax.optimization_barrier(jnp.sum(final_prob * (final_logits - logits), axis=-1)) - final_lse + lse)
    logprobs.append(jnp.take_along_axis(final_logits, wanted, axis=1)[:, 0] - final_lse)
    logprob = jnp.where(live[None, :], jnp.stack(logprobs), 0.0).reshape(LAYERS + 1, seqs, CAP)
    divergence = jnp.where(live[None, :], jnp.stack(divergences), 0.0).reshape(LAYERS, seqs, CAP)
    return (logprob, divergence)
```

```python
import jax
import jax.numpy as jnp
from jax import lax
from jax.experimental import pallas as pl
from jax.experimental.pallas import tpu as pltpu
from jax.sharding import Mesh
from jax.sharding import PartitionSpec as P

D = 6144
LAYERS = 3
CAP = 32
ROWS = 256
SEQ = ("z", "c")
VOCAB = ("y", "x")
F32 = jnp.float32
BF16 = jnp.bfloat16
NT = (((1,), (1,)), ((), ()))
TN = (((0,), (0,)), ((), ()))
INFO = 128
SHIFT = 16.0


def dot(a, b):
    return jnp.dot(a, b, preferred_element_type=F32)


def exchange(value, axes):
    return lax.all_to_all(value, axes, split_axis=0, concat_axis=0, tiled=True)


def swap_cores(value):
    return lax.ppermute(value, "c", [(0, 1), (1, 0)])


def whole(shape, dtype):
    return jax.ShapeDtypeStruct(shape, dtype)


def translate_kernel(flags, own, other, translator, out):
    low_core = flags[0] == 0
    keep = flags[1].astype(F32)
    lane = lax.broadcasted_iota(jnp.int32, (CAP, ROWS), 1).astype(F32)
    slot = lax.broadcasted_iota(jnp.int32, (CAP, ROWS), 0).astype(F32)
    base = jnp.zeros((1, 1), F32)
    pick_own, pick_other = [], []
    for k in range(8):
        count_own = own[k, INFO + 2 : INFO + 3, 0:1].astype(F32)
        count_other = other[k, INFO + 2 : INFO + 3, 0:1].astype(F32)
        start_own = base + jnp.where(low_core, 0.0, count_other)
        start_other = base + jnp.where(low_core, count_own, 0.0)
        hit_own = (lane == start_own + slot) & (slot < count_own)
        hit_other = (lane == start_other + slot) & (slot < count_other)
        pick_own.append(jnp.where(hit_own, 1.0, 0.0).astype(BF16))
        pick_other.append(jnp.where(hit_other, 1.0, 0.0).astype(BF16))
        base = base + count_own + count_other
    pick_own = jnp.concatenate(pick_own, axis=0)
    pick_other = jnp.concatenate(pick_other, axis=0)
    for layer in range(LAYERS + 1):
        low = layer * CAP
        a = own[:, low : low + CAP, :].reshape(ROWS, -1)
        b = other[:, low : low + CAP, :].reshape(ROWS, -1)
        rows = lax.dot_general(pick_own, a, TN, preferred_element_type=F32)
        rows = rows + lax.dot_general(pick_other, b, TN, preferred_element_type=F32)
        part = rows * keep
        if layer < LAYERS:
            part = part + dot(rows.astype(BF16), translator[layer])
        out[:, layer] = part.astype(BF16).reshape(16, 16, -1)


def high_low(value):
    high = value.astype(BF16).astype(F32)
    row = lax.broadcasted_iota(jnp.int32, value.shape, 0)
    return jnp.where(row == 0, high, jnp.where(row == 1, value - high, 0.0))


def scale_kernel(parts, bias, gain, y_out):
    x = parts[0].astype(F32)
    for k in range(1, 16):
        x = x + parts[k].astype(F32)
    x = x + bias[...]
    y = (x * gain[...]).astype(BF16)
    square = x * x
    square = jnp.concatenate([square, square], axis=0)
    ones = jnp.ones((8, x.shape[1]), F32)
    squares = lax.dot_general(ones, square, NT, precision=lax.Precision.HIGHEST, preferred_element_type=F32)
    squares = high_low(squares)
    for k in range(16):
        y_out[k, 0:64] = y
        y_out[k, 64:72] = jnp.zeros((8, x.shape[1]), BF16)
        y_out[k, 64:72, 0:128] = squares.astype(BF16)


def logits_kernel(y_own, y_other, u_own, u_other, out):
    a = y_own[:, 0:64, :].reshape(1024, -1)
    b = y_other[:, 0:64, :].reshape(1024, -1)
    part = lax.dot_general(a, u_own[...], NT, preferred_element_type=F32)
    part = part + lax.dot_general(b, u_other[...], NT, preferred_element_type=F32)
    out[:, 0:128, :] = (part * (1.0 / SHIFT)).reshape(8, 128, -1)
    out[:, 128:136, :] = jnp.zeros((8, 8, out.shape[2]), F32)

    @pl.when(pl.program_id(0) == 0)
    def _():
        lane = lax.broadcasted_iota(jnp.int32, (8, 128), 1)
        sums = []
        for k in range(16):
            four = y_own[k, 64:72, 0:128].astype(F32) + y_other[k, 64:72, 0:128].astype(F32)
            sums.append(jnp.broadcast_to(four[0:1] + four[1:2], (8, 128)))
        for k in range(8):
            norm = jnp.sqrt(jnp.where(lane < 64, sums[2 * k], sums[2 * k + 1]))
            out[k, 128:136, 0:128] = high_low(norm * (1.0 / SHIFT))


def stats_kernel(summed, norms, target, out):
    square = jnp.zeros((1, 128), F32)
    for k in range(8):
        norm = norms[k, 0:1] + norms[k, 1:2]
        square = square + norm * norm
    factor = SHIFT * lax.rsqrt(square * (SHIFT * SHIFT / D) + 1e-05)
    factor = jnp.broadcast_to(factor, (128, 128)).T[:, 0:1]
    logits = summed[...] * factor
    width = logits.shape[1]
    expz = jnp.exp(logits)
    total = jnp.sum(expz, axis=1, keepdims=True)
    ids = lax.broadcasted_iota(jnp.int32, logits.shape, 1)
    picked = jnp.sum(jnp.where(ids == target[...], logits, 0.0), axis=1, keepdims=True)
    four = logits.reshape(2, 4, 16, width)
    last = expz.reshape(2, 4, 16, width)[:, 3:]
    cross = jnp.sum(last * (four[:, 3:] - four), axis=3, keepdims=True).reshape(128, 1)
    lane = lax.broadcasted_iota(jnp.int32, (128, 128), 1)
    table = jnp.where(lane == 0, total, jnp.where(lane == 1, cross, jnp.where(lane == 2, picked, 0.0)))
    rows = table.T[:8]
    for k in range(32):
        out[k] = rows


def body(
    probe_states,
    final_states,
    translator,
    translator_bias,
    norm_gain,
    unembed,
    answer_rows,
    answer_count,
    targets,
):
    z = lax.axis_index("z")
    c = lax.axis_index("c")
    v = lax.axis_index(VOCAB)
    seq = 2 * z + c
    width = probe_states.shape[2]
    half = unembed.shape[0] // 2
    picks = answer_rows[0]

    u_own = lax.dynamic_slice_in_dim(unembed, c * half, half, 0)
    u_other = swap_cores(lax.dynamic_slice_in_dim(unembed, (1 - c) * half, half, 0))

    info = jnp.concatenate(
        [targets // 256, targets % 256, jnp.broadcast_to(answer_count[:, None], (1, CAP)), jnp.zeros((5, CAP), jnp.int32)]
    )
    info = jnp.pad(info, ((0, 0), (0, width - CAP))).astype(BF16)
    local = jnp.concatenate(
        [
            jnp.take(probe_states, picks, axis=1, mode="clip").reshape(LAYERS * CAP, width),
            jnp.take(final_states, picks, axis=0, mode="clip"),
            info,
        ],
        axis=0,
    )
    own = exchange(jnp.broadcast_to(local[None], (8, *local.shape)), "z")
    other = swap_cores(own)

    flags = jnp.stack([c, (seq == v).astype(jnp.int32)])
    parts = pl.pallas_call(
        translate_kernel,
        out_shape=whole((16, 4, 16, width), BF16),
        in_specs=[pl.BlockSpec(memory_space=pltpu.SMEM)] + [pl.BlockSpec(memory_space=pltpu.VMEM)] * 3,
        name="translate",
    )(flags, own, other, translator)
    arrived = exchange(parts.reshape(16, 64, width), VOCAB)

    bias = jnp.concatenate([translator_bias, jnp.zeros((1, width), F32)], axis=0)
    bias = jnp.repeat(bias, 16, axis=0)
    y_copies = pl.pallas_call(scale_kernel, out_shape=whole((16, 72, width), BF16), name="scale")(
        arrived, bias, norm_gain[None, :]
    )
    y_own = exchange(y_copies, VOCAB)
    y_other = swap_cores(y_own)

    block = 256
    product = pl.pallas_call(
        logits_kernel,
        grid=(half // block,),
        in_specs=[
            pl.BlockSpec((16, 72, width), lambda i: (0, 0, 0)),
            pl.BlockSpec((16, 72, width), lambda i: (0, 0, 0)),
            pl.BlockSpec((block, width), lambda i: (i, 0)),
            pl.BlockSpec((block, width), lambda i: (i, 0)),
        ],
        out_specs=pl.BlockSpec((8, 136, block), lambda i: (0, 0, i)),
        out_shape=whole((8, 136, half), F32),
        name="logits",
    )(y_own, y_other, u_own, u_other)
    info_own, info_other, product = lax.optimization_barrier(
        (own[:, INFO : INFO + 8, :CAP], other[:, INFO : INFO + 8, :CAP], product)
    )
    logit_parts = exchange(product.astype(jnp.float16), "z")
    norms = logit_parts[:, 128:136, :128].astype(F32)
    summed = jnp.sum(logit_parts[:, :128].astype(F32), axis=0)

    info_own = info_own.astype(jnp.int32)
    info_other = info_other.astype(jnp.int32)
    every_info = jnp.stack(
        [jnp.where(c == 0, info_own, info_other), jnp.where(c == 0, info_other, info_own)], axis=1
    ).reshape(16, 8, CAP)
    counts = every_info[:, 2, 0]
    all_targets = every_info[:, 0] * 256 + every_info[:, 1]
    order = jnp.arange(16, dtype=jnp.int32)
    starts = jnp.sum(jnp.where(order[None, :] < order[:, None], counts[None, :], 0), axis=1)
    slots = jnp.arange(CAP, dtype=jnp.int32)
    place = jnp.where(slots[None, :] < counts[:, None], starts[:, None] + slots[None, :], -1)
    row_ids = z * 32 + jnp.arange(32, dtype=jnp.int32)
    hit = place[None] == row_ids[:, None, None]
    row_targets = jnp.sum(jnp.where(hit, all_targets[None], 0), axis=(1, 2))
    local_targets = row_targets - (v * 2 + c) * half
    item_targets = jnp.broadcast_to(local_targets.reshape(2, 1, 16), (2, 4, 16)).reshape(128, 1)
    stats = pl.pallas_call(stats_kernel, out_shape=whole((32, 8, 128), F32), name="stats")(
        summed, norms, item_targets
    )
    sums = jnp.sum(exchange(stats, ("c", "y", "x")), axis=0)
    every = exchange(jnp.broadcast_to(sums[None], (8, 8, 128)), "z")

    table = every[:, :3].reshape(8, 3, 2, 4, 16).transpose(1, 3, 0, 2, 4).reshape(3, 4, 1, ROWS)
    my_start = jnp.sum(jnp.where(order == seq, starts, 0))
    live = slots < answer_count[0]
    wanted = my_start + slots
    mine = wanted[:, None] == jnp.arange(ROWS, dtype=jnp.int32)[None, :]
    mine = jnp.sum(jnp.where(mine[None, None], table, 0.0), axis=3)
    log_total = jnp.log(mine[0])
    logprob = mine[2] - log_total
    divergence = mine[1, :LAYERS] / mine[0, LAYERS:] - log_total[LAYERS:] + log_total[:LAYERS]
    logprob = jnp.where(live[None], logprob, 0.0)[:, None, :]
    divergence = jnp.where(live[None], divergence, 0.0)[:, None, :]
    return (logprob, divergence)


def solution(mesh):
    split = Mesh(mesh.devices.reshape(8, 2, 4, 4), ("z", "c", "y", "x"))
    return jax.shard_map(
        body,
        mesh=split,
        in_specs=(
            P(None, SEQ, VOCAB),
            P(SEQ, VOCAB),
            P(None, VOCAB, SEQ),
            P(None, SEQ),
            P(SEQ),
            P(VOCAB, SEQ),
            P(SEQ, None),
            P(SEQ),
            P(SEQ, None),
        ),
        out_specs=(P(None, SEQ, None), P(None, SEQ, None)),
        check_vma=False,
    )
```

```python
import jax
import jax.numpy as jnp
from jax import lax
from jax.experimental import pallas as pl
from jax.experimental.pallas import tpu as pltpu
from jax.sharding import Mesh
from jax.sharding import PartitionSpec as P


D = 6144
LAYERS = 3
CAP = 32
ROWS = 256
Z = ("zq", "zp")
SEQ = ("zq", "zp", "c")
VOCAB = ("y", "x")
F32 = jnp.float32
BF16 = jnp.bfloat16
NT = (((1,), (1,)), ((), ()))
TN = (((0,), (0,)), ((), ()))
INFO = 128
SHIFT = 16.0


def dot(a, b):
    return jnp.dot(a, b, preferred_element_type=F32)


def exchange(value, axes):
    return lax.all_to_all(value, axes, split_axis=0, concat_axis=0, tiled=True)


def swap_cores(value):
    return lax.ppermute(value, "c", [(0, 1), (1, 0)])


def whole(shape, dtype):
    return jax.ShapeDtypeStruct(shape, dtype)


def translate_kernel(flags, own, other, translator, out, info):
    low_core = flags[0] == 0
    keep = flags[1].astype(F32)
    lane = lax.broadcasted_iota(jnp.int32, (CAP, ROWS), 1).astype(F32)
    slot = lax.broadcasted_iota(jnp.int32, (CAP, ROWS), 0).astype(F32)
    base = jnp.zeros((1, 1), F32)
    pick_own, pick_other = [], []
    for k in range(8):
        count_own = own[k, INFO + 2 : INFO + 3, 0:1].astype(F32)
        count_other = other[k, INFO + 2 : INFO + 3, 0:1].astype(F32)
        start_own = base + jnp.where(low_core, 0.0, count_other)
        start_other = base + jnp.where(low_core, count_own, 0.0)
        hit_own = (lane == start_own + slot) & (slot < count_own)
        hit_other = (lane == start_other + slot) & (slot < count_other)
        pick_own.append(jnp.where(hit_own, 1.0, 0.0).astype(BF16))
        pick_other.append(jnp.where(hit_other, 1.0, 0.0).astype(BF16))
        base = base + count_own + count_other
        a = own[k, INFO : INFO + 8, 0:128].astype(F32)
        b = other[k, INFO : INFO + 8, 0:128].astype(F32)
        info[2 * k] = jnp.where(low_core, a, b)
        info[2 * k + 1] = jnp.where(low_core, b, a)
    pick_own = jnp.concatenate(pick_own, axis=0)
    pick_other = jnp.concatenate(pick_other, axis=0)
    for layer in range(LAYERS + 1):
        low = layer * CAP
        a = own[:, low : low + CAP, :].reshape(ROWS, -1)
        b = other[:, low : low + CAP, :].reshape(ROWS, -1)
        rows = lax.dot_general(pick_own, a, TN, preferred_element_type=F32)
        rows = rows + lax.dot_general(pick_other, b, TN, preferred_element_type=F32)
        part = rows * keep
        if layer < LAYERS:
            part = part + dot(rows.astype(BF16), translator[layer])
        out[:, layer] = part.astype(BF16).reshape(16, 16, -1)


def high_low(value):
    high = value.astype(BF16).astype(F32)
    row = lax.broadcasted_iota(jnp.int32, value.shape, 0)
    return jnp.where(row == 0, high, jnp.where(row == 1, value - high, 0.0))


def scale_kernel(parts, bias, gain, y_out):
    x = parts[0].astype(F32)
    for k in range(1, 16):
        x = x + parts[k].astype(F32)
    x = x + bias[...]
    y = (x * gain[...]).astype(BF16)
    square = x * x
    square = jnp.concatenate([square] * 4, axis=0)
    ones = jnp.ones((8, x.shape[1]), F32)
    squares = lax.dot_general(ones, square, NT, precision=lax.Precision.HIGHEST, preferred_element_type=F32)
    squares = high_low(squares)
    for k in range(32):
        y_out[k, 0:64] = y
        y_out[k, 64:72] = jnp.zeros((8, x.shape[1]), BF16)
        y_out[k, 64:72, 0:256] = squares.astype(BF16)


def logits_kernel(flags, y_own, y_other, u0, u1, u2, u3, out):
    pair = flags[2]
    part = jnp.zeros((1024, u0.shape[0]), F32)
    for k in range(2):
        at = pl.ds(16 * (pair if k == 0 else 1 - pair), 16)
        a = y_own[at, 0:64, :].reshape(1024, -1)
        b = y_other[at, 0:64, :].reshape(1024, -1)
        part = part + lax.dot_general(a, (u0, u2)[k][...], NT, preferred_element_type=F32)
        part = part + lax.dot_general(b, (u1, u3)[k][...], NT, preferred_element_type=F32)
    out[:, 0:256, :] = (part * (1.0 / SHIFT)).reshape(4, 256, -1)
    out[:, 256:264, :] = jnp.zeros((4, 8, out.shape[2]), F32)
    lane = lax.broadcasted_iota(jnp.int32, (8, 256), 1)
    for k in range(4):
        square = jnp.zeros((8, 256), F32)
        for j in range(4):
            total = jnp.zeros((1, 256), F32)
            for half in range(2):
                at = 16 * half + 4 * k + j
                both = y_own[at, 64:72, 0:256].astype(F32) + y_other[at, 64:72, 0:256].astype(F32)
                total = total + both[0:1] + both[1:2]
            square = jnp.where(lane // 64 == j, jnp.broadcast_to(total, (8, 256)), square)
        out[k, 256:264, 0:256] = high_low(jnp.sqrt(square) * (1.0 / SHIFT))


def stats_kernel(summed, norms, target, out):
    square = jnp.zeros((1, 256), F32)
    for k in range(4):
        norm = norms[k, 0:1] + norms[k, 1:2]
        square = square + norm * norm
    factor = SHIFT * lax.rsqrt(square * (SHIFT * SHIFT / D) + 1e-05)
    factor = jnp.broadcast_to(factor, (128, 256)).T[:, 0:1]
    logits = summed[...] * factor
    width = logits.shape[1]
    expz = jnp.exp(logits)
    total = jnp.sum(expz, axis=1, keepdims=True)
    ids = lax.broadcasted_iota(jnp.int32, logits.shape, 1)
    picked = jnp.sum(jnp.where(ids == target[...], logits, 0.0), axis=1, keepdims=True)
    four = logits.reshape(4, 4, 16, width)
    last = expz.reshape(4, 4, 16, width)[:, 3:]
    cross = jnp.sum(last * (four[:, 3:] - four), axis=3, keepdims=True).reshape(256, 1)
    lane = lax.broadcasted_iota(jnp.int32, (256, 128), 1)
    table = jnp.where(lane == 0, total, jnp.where(lane == 1, cross, jnp.where(lane == 2, picked, 0.0)))
    rows = table.T[:8]
    for k in range(64):
        out[k] = rows


def body(
    probe_states,
    final_states,
    translator,
    translator_bias,
    norm_gain,
    unembed,
    answer_rows,
    answer_count,
    targets,
):
    zq = lax.axis_index("zq")
    c = lax.axis_index("c")
    quarter = 2 * lax.axis_index("zp") + c
    v = lax.axis_index(VOCAB)
    seq = 4 * zq + quarter
    width = probe_states.shape[2]
    part = unembed.shape[0] // 4
    picks = answer_rows[0]

    info = jnp.concatenate(
        [targets // 256, targets % 256, jnp.broadcast_to(answer_count[:, None], (1, CAP)), jnp.zeros((5, CAP), jnp.int32)]
    )
    info = jnp.pad(info, ((0, 0), (0, width - CAP))).astype(BF16)
    local = jnp.concatenate(
        [
            jnp.take(probe_states, picks, axis=1, mode="clip").reshape(LAYERS * CAP, width),
            jnp.take(final_states, picks, axis=0, mode="clip"),
            info,
        ],
        axis=0,
    )
    own = exchange(jnp.broadcast_to(local[None], (8, *local.shape)), Z)
    other = swap_cores(own)

    flags = jnp.stack([c, (seq == v).astype(jnp.int32), quarter // 2])
    parts, every_info = pl.pallas_call(
        translate_kernel,
        out_shape=(whole((16, 4, 16, width), BF16), whole((16, 8, 128), F32)),
        in_specs=[pl.BlockSpec(memory_space=pltpu.SMEM)] + [pl.BlockSpec(memory_space=pltpu.VMEM)] * 3,
        name="translate",
    )(flags, own, other, translator)
    arrived = exchange(parts.reshape(16, 64, width), VOCAB)
    fours = unembed.reshape(4, part, width)
    quarters = []
    for k in range(4):
        block = lax.dynamic_index_in_dim(fours, quarter ^ k, 0, keepdims=False)
        if k:
            block = lax.ppermute(block, ("zp", "c"), [(j, j ^ k) for j in range(4)])
        quarters.append(block)

    bias = jnp.concatenate([translator_bias, jnp.zeros((1, width), F32)], axis=0)
    bias = jnp.repeat(bias, 16, axis=0)
    y_copies = pl.pallas_call(scale_kernel, out_shape=whole((32, 72, width), BF16), name="scale")(
        arrived, bias, norm_gain[None, :]
    )
    y_own = exchange(y_copies, ("zp", *VOCAB))
    y_other = swap_cores(y_own)

    product = pl.pallas_call(
        logits_kernel,
        out_shape=whole((4, 264, part), F32),
        in_specs=[pl.BlockSpec(memory_space=pltpu.SMEM)] + [pl.BlockSpec(memory_space=pltpu.VMEM)] * 6,
        name="logits",
    )(flags, y_own, y_other, *quarters)
    every_info, product = lax.optimization_barrier((every_info, product))
    logit_parts = exchange(product.astype(jnp.float16), "zq")
    norms = logit_parts[:, 256:264, :256].astype(F32)
    summed = jnp.sum(logit_parts[:, :256].astype(F32), axis=0)

    every_info = every_info[:, :3, :CAP].astype(jnp.int32)
    counts = every_info[:, 2, 0]
    all_targets = every_info[:, 0] * 256 + every_info[:, 1]
    order = jnp.arange(16, dtype=jnp.int32)
    starts = jnp.sum(jnp.where(order[None, :] < order[:, None], counts[None, :], 0), axis=1)
    slots = jnp.arange(CAP, dtype=jnp.int32)
    place = jnp.where(slots[None, :] < counts[:, None], starts[:, None] + slots[None, :], -1)
    row_ids = zq * 64 + jnp.arange(64, dtype=jnp.int32)
    hit = place[None] == row_ids[:, None, None]
    row_targets = jnp.sum(jnp.where(hit, all_targets[None], 0), axis=(1, 2))
    local_targets = row_targets - (v * 4 + quarter) * part
    item_targets = jnp.broadcast_to(local_targets.reshape(4, 1, 16), (4, 4, 16)).reshape(256, 1)
    stats = pl.pallas_call(stats_kernel, out_shape=whole((64, 8, 256), F32), name="stats")(
        summed, norms, item_targets
    )
    sums = jnp.sum(exchange(stats, ("zp", "c", *VOCAB)), axis=0)
    every = exchange(jnp.broadcast_to(sums[None], (4, 8, 256)), "zq")

    table = every[:, :3].reshape(4, 3, 4, 4, 16).transpose(1, 3, 0, 2, 4).reshape(3, 4, 1, ROWS)
    my_start = jnp.sum(jnp.where(order == seq, starts, 0))
    live = slots < answer_count[0]
    wanted = my_start + slots
    mine = wanted[:, None] == jnp.arange(ROWS, dtype=jnp.int32)[None, :]
    mine = jnp.sum(jnp.where(mine[None, None], table, 0.0), axis=3)
    log_total = jnp.log(mine[0])
    logprob = mine[2] - log_total
    divergence = mine[1, :LAYERS] / mine[0, LAYERS:] - log_total[LAYERS:] + log_total[:LAYERS]
    logprob = jnp.where(live[None], logprob, 0.0)[:, None, :]
    divergence = jnp.where(live[None], divergence, 0.0)[:, None, :]
    return (logprob, divergence)


def solution(mesh):
    split = Mesh(mesh.devices.reshape(4, 2, 2, 4, 4), ("zq", "zp", "c", "y", "x"))
    return jax.shard_map(
        body,
        mesh=split,
        in_specs=(
            P(None, SEQ, VOCAB),
            P(SEQ, VOCAB),
            P(None, VOCAB, SEQ),
            P(None, SEQ),
            P(SEQ),
            P(VOCAB, SEQ),
            P(SEQ, None),
            P(SEQ),
            P(SEQ, None),
        ),
        out_specs=(P(None, SEQ, None), P(None, SEQ, None)),
        check_vma=False,
    )
```

```python
import jax
import jax.numpy as jnp
from jax import lax
from jax.experimental import pallas as pl
from jax.experimental.pallas import tpu as pltpu
from jax.sharding import Mesh
from jax.sharding import PartitionSpec as P


D = 6144
LAYERS = 3
CAP = 32
ROWS = 256
Z = ("zq", "zp")
SEQ = ("zq", "zp", "c")
VOCAB = ("y", "x")
F32 = jnp.float32
BF16 = jnp.bfloat16
NT = (((1,), (1,)), ((), ()))
TN = (((0,), (0,)), ((), ()))
INFO = 128
SHIFT = 16.0


def dot(a, b):
    return jnp.dot(a, b, preferred_element_type=F32)


def exchange(value, axes):
    return lax.all_to_all(value, axes, split_axis=0, concat_axis=0, tiled=True)


def swap_cores(value):
    return lax.ppermute(value, "c", [(0, 1), (1, 0)])


def whole(shape, dtype):
    return pltpu.VMEM(shape, dtype)


def far(shape, dtype):
    return jax.ShapeDtypeStruct(shape, dtype)


def near(value):
    return pltpu.with_memory_space_constraint(value, pltpu.VMEM)


SCALARS = pl.BlockSpec(memory_space=pltpu.SMEM)
VECTORS = pl.BlockSpec(memory_space=pltpu.VMEM)
LIMIT = pltpu.CompilerParams(vmem_limit_bytes=24 * 1024 * 1024)


def translate_kernel(flags, own, other, translator, out, info):
    low_core = flags[0] == 0
    keep = flags[1].astype(F32)
    lane = lax.broadcasted_iota(jnp.int32, (CAP, ROWS), 1).astype(F32)
    slot = lax.broadcasted_iota(jnp.int32, (CAP, ROWS), 0).astype(F32)
    base = jnp.zeros((1, 1), F32)
    pick_own, pick_other = [], []
    for k in range(8):
        count_own = own[k, INFO + 2 : INFO + 3, 0:1].astype(F32)
        count_other = other[k, INFO + 2 : INFO + 3, 0:1].astype(F32)
        start_own = base + jnp.where(low_core, 0.0, count_other)
        start_other = base + jnp.where(low_core, count_own, 0.0)
        hit_own = (lane == start_own + slot) & (slot < count_own)
        hit_other = (lane == start_other + slot) & (slot < count_other)
        pick_own.append(jnp.where(hit_own, 1.0, 0.0).astype(BF16))
        pick_other.append(jnp.where(hit_other, 1.0, 0.0).astype(BF16))
        base = base + count_own + count_other
        a = own[k, INFO : INFO + 8, 0:128].astype(F32)
        b = other[k, INFO : INFO + 8, 0:128].astype(F32)
        info[2 * k] = jnp.where(low_core, a, b)
        info[2 * k + 1] = jnp.where(low_core, b, a)
    pick_own = jnp.concatenate(pick_own, axis=0)
    pick_other = jnp.concatenate(pick_other, axis=0)
    for layer in range(LAYERS + 1):
        low = layer * CAP
        a = own[:, low : low + CAP, :].reshape(ROWS, -1)
        b = other[:, low : low + CAP, :].reshape(ROWS, -1)
        rows = lax.dot_general(pick_own, a, TN, preferred_element_type=F32)
        rows = rows + lax.dot_general(pick_other, b, TN, preferred_element_type=F32)
        part = rows * keep
        if layer < LAYERS:
            part = part + dot(rows.astype(BF16), translator[layer])
        out[:, layer] = part.astype(BF16).reshape(16, 16, -1)


def high_low(value):
    high = value.astype(BF16).astype(F32)
    row = lax.broadcasted_iota(jnp.int32, value.shape, 0)
    return jnp.where(row == 0, high, jnp.where(row == 1, value - high, 0.0))


def scale_kernel(parts, bias, gain, y_out):
    x = parts[0].astype(F32)
    for k in range(1, 16):
        x = x + parts[k].astype(F32)
    x = x + bias[...]
    y = (x * gain[...]).astype(BF16)
    square = x * x
    square = jnp.concatenate([square] * 4, axis=0)
    ones = jnp.ones((8, x.shape[1]), F32)
    squares = lax.dot_general(ones, square, NT, precision=lax.Precision.HIGHEST, preferred_element_type=F32)
    squares = high_low(squares)
    for k in range(32):
        y_out[k, 0:64] = y
        y_out[k, 64:72] = jnp.zeros((8, x.shape[1]), BF16)
        y_out[k, 64:72, 0:256] = squares.astype(BF16)


def logits_kernel(flags, y_own, y_other, u0, u1, u2, u3, out):
    pair = flags[2]
    part = jnp.zeros((1024, u0.shape[0]), F32)
    for k in range(2):
        at = pl.ds(16 * (pair if k == 0 else 1 - pair), 16)
        a = y_own[at, 0:64, :].reshape(1024, -1)
        b = y_other[at, 0:64, :].reshape(1024, -1)
        part = part + lax.dot_general(a, (u0, u2)[k][...], NT, preferred_element_type=F32)
        part = part + lax.dot_general(b, (u1, u3)[k][...], NT, preferred_element_type=F32)
    out[:, 0:256, :] = (part * (1.0 / SHIFT)).reshape(4, 256, -1)
    out[:, 256:264, :] = jnp.zeros((4, 8, out.shape[2]), F32)
    lane = lax.broadcasted_iota(jnp.int32, (8, 256), 1)
    for k in range(4):
        square = jnp.zeros((8, 256), F32)
        for j in range(4):
            total = jnp.zeros((1, 256), F32)
            for half in range(2):
                at = 16 * half + 4 * k + j
                both = y_own[at, 64:72, 0:256].astype(F32) + y_other[at, 64:72, 0:256].astype(F32)
                total = total + both[0:1] + both[1:2]
            square = jnp.where(lane // 64 == j, jnp.broadcast_to(total, (8, 256)), square)
        out[k, 256:264, 0:256] = high_low(jnp.sqrt(square) * (1.0 / SHIFT))


def stats_kernel(summed, norms, target, out):
    square = jnp.zeros((1, 256), F32)
    for k in range(4):
        norm = norms[k, 0:1] + norms[k, 1:2]
        square = square + norm * norm
    factor = SHIFT * lax.rsqrt(square * (SHIFT * SHIFT / D) + 1e-05)
    factor = jnp.broadcast_to(factor, (128, 256)).T[:, 0:1]
    logits = summed[...] * factor
    width = logits.shape[1]
    expz = jnp.exp(logits)
    total = jnp.sum(expz, axis=1, keepdims=True)
    ids = lax.broadcasted_iota(jnp.int32, logits.shape, 1)
    picked = jnp.sum(jnp.where(ids == target[...], logits, 0.0), axis=1, keepdims=True)
    four = logits.reshape(4, 4, 16, width)
    last = expz.reshape(4, 4, 16, width)[:, 3:]
    cross = jnp.sum(last * (four[:, 3:] - four), axis=3, keepdims=True).reshape(256, 1)
    lane = lax.broadcasted_iota(jnp.int32, (128, 128), 1)
    table = jnp.zeros((128, 128), F32)
    for h in range(2):
        for k, value in enumerate((total, cross, picked)):
            table = jnp.where(lane == 3 * h + k, value[128 * h : 128 * h + 128], table)
    rows = table.T[:8]
    for k in range(64):
        out[k] = rows


def body(
    probe_states,
    final_states,
    translator,
    translator_bias,
    norm_gain,
    unembed,
    answer_rows,
    answer_count,
    targets,
):
    zq = lax.axis_index("zq")
    c = lax.axis_index("c")
    quarter = 2 * lax.axis_index("zp") + c
    v = lax.axis_index(VOCAB)
    seq = 4 * zq + quarter
    width = probe_states.shape[2]
    part = unembed.shape[0] // 4
    picks = answer_rows[0]

    info = jnp.concatenate(
        [targets // 256, targets % 256, jnp.broadcast_to(answer_count[:, None], (1, CAP)), jnp.zeros((5, CAP), jnp.int32)]
    )
    info = jnp.pad(info, ((0, 0), (0, width - CAP))).astype(BF16)
    local = jnp.concatenate(
        [
            jnp.take(probe_states, picks, axis=1, mode="clip").reshape(LAYERS * CAP, width),
            jnp.take(final_states, picks, axis=0, mode="clip"),
            info,
        ],
        axis=0,
    )
    own = exchange(jnp.broadcast_to(local[None], (8, *local.shape)), Z)
    other = swap_cores(own)

    flags = jnp.stack([c, (seq == v).astype(jnp.int32), quarter // 2])
    parts, every_info = pl.pallas_call(
        translate_kernel,
        out_shape=(far((16, 4, 16, width), BF16), far((16, 8, 128), F32)),
        in_specs=[SCALARS] + [VECTORS] * 3,
        out_specs=(VECTORS, VECTORS),
        compiler_params=LIMIT,
        name="translate",
    )(flags, near(own), near(other), translator)
    arrived = exchange(parts.reshape(16, 64, width), VOCAB)
    fours = unembed.reshape(4, part, width)
    quarters = []
    for k in range(4):
        block = lax.dynamic_index_in_dim(fours, quarter ^ k, 0, keepdims=False)
        if k:
            block = lax.ppermute(block, ("zp", "c"), [(j, j ^ k) for j in range(4)])
        quarters.append(block)

    bias = jnp.concatenate([translator_bias, jnp.zeros((1, width), F32)], axis=0)
    bias = jnp.repeat(bias, 16, axis=0)
    y_copies = pl.pallas_call(
        scale_kernel,
        out_shape=whole((32, 72, width), BF16),
        in_specs=[VECTORS] * 3,
        out_specs=VECTORS,
        compiler_params=LIMIT,
        name="scale",
    )(near(arrived), bias, norm_gain[None, :])
    y_own = exchange(y_copies, ("zp", *VOCAB))
    y_other = swap_cores(y_own)

    product = pl.pallas_call(
        logits_kernel,
        out_shape=whole((4, 264, part), F32),
        in_specs=[SCALARS] + [VECTORS] * 6,
        out_specs=VECTORS,
        compiler_params=LIMIT,
        name="logits",
    )(flags, near(y_own), near(y_other), *[near(block) for block in quarters])
    every_info, product = lax.optimization_barrier((every_info, product))
    logit_parts = exchange(product.astype(jnp.float16), "zq")
    norms = logit_parts[:, 256:264, :256].astype(F32)
    summed = jnp.sum(logit_parts[:, :256].astype(F32), axis=0)

    every_info = every_info[:, :3, :CAP].astype(jnp.int32)
    counts = every_info[:, 2, 0]
    all_targets = every_info[:, 0] * 256 + every_info[:, 1]
    order = jnp.arange(16, dtype=jnp.int32)
    starts = jnp.sum(jnp.where(order[None, :] < order[:, None], counts[None, :], 0), axis=1)
    slots = jnp.arange(CAP, dtype=jnp.int32)
    place = jnp.where(slots[None, :] < counts[:, None], starts[:, None] + slots[None, :], -1)
    row_ids = zq * 64 + jnp.arange(64, dtype=jnp.int32)
    hit = place[None] == row_ids[:, None, None]
    row_targets = jnp.sum(jnp.where(hit, all_targets[None], 0), axis=(1, 2))
    local_targets = row_targets - (v * 4 + quarter) * part
    item_targets = jnp.broadcast_to(local_targets.reshape(4, 1, 16), (4, 4, 16)).reshape(256, 1)
    stats = pl.pallas_call(
        stats_kernel,
        out_shape=far((64, 8, 128), F32),
        in_specs=[VECTORS] * 3,
        out_specs=VECTORS,
        compiler_params=LIMIT,
        name="stats",
    )(near(summed), near(norms), item_targets)
    sums = jnp.sum(exchange(stats, ("zp", "c", *VOCAB)), axis=0)
    every = [sums]
    for k in (1, 2, 3):
        every.append(lax.ppermute(sums, "zq", [(j, (j + k) % 4) for j in range(4)]))
    every = jnp.stack(every)

    table = every[:, :6].reshape(4, 2, 3, 2, 4, 16).transpose(2, 4, 0, 1, 3, 5).reshape(3, 4, 1, ROWS)
    chunk = (zq - jnp.arange(4, dtype=jnp.int32)) % 4
    held = (chunk[:, None] * 64 + jnp.arange(64, dtype=jnp.int32)[None, :]).reshape(1, ROWS)
    my_start = jnp.sum(jnp.where(order == seq, starts, 0))
    live = slots < answer_count[0]
    wanted = my_start + slots
    mine = wanted[:, None] == held
    mine = jnp.sum(jnp.where(mine[None, None], table, 0.0), axis=3)
    log_total = jnp.log(mine[0])
    logprob = mine[2] - log_total
    divergence = mine[1, :LAYERS] / mine[0, LAYERS:] - log_total[LAYERS:] + log_total[:LAYERS]
    logprob = jnp.where(live[None], logprob, 0.0)[:, None, :]
    divergence = jnp.where(live[None], divergence, 0.0)[:, None, :]
    return (logprob, divergence)


def solution(mesh):
    split = Mesh(mesh.devices.reshape(4, 2, 2, 4, 4), ("zq", "zp", "c", "y", "x"))
    return jax.shard_map(
        body,
        mesh=split,
        in_specs=(
            P(None, SEQ, VOCAB),
            P(SEQ, VOCAB),
            P(None, VOCAB, SEQ),
            P(None, SEQ),
            P(SEQ),
            P(VOCAB, SEQ),
            P(SEQ, None),
            P(SEQ),
            P(SEQ, None),
        ),
        out_specs=(P(None, SEQ, None), P(None, SEQ, None)),
        check_vma=False,
    )
```

```python
import functools

import jax
import jax.numpy as jnp
from jax import lax
from jax.experimental import pallas as pl
from jax.experimental.pallas import tpu as pltpu
from jax.sharding import Mesh
from jax.sharding import PartitionSpec as P


D = 6144
LAYERS = 3
CAP = 32
ROWS = 256
Z = ("zq", "zp")
SEQ = ("zq", "zp", "c")
VOCAB = ("y", "x")
F32 = jnp.float32
BF16 = jnp.bfloat16
NT = (((1,), (1,)), ((), ()))
TN = (((0,), (0,)), ((), ()))
INFO = 128
SHIFT = 16.0
SCALE = 262144.0
LARGE = 16.0


def dot(a, b):
    return jnp.dot(a, b, preferred_element_type=F32)


def exchange(value, axes):
    return lax.all_to_all(value, axes, split_axis=0, concat_axis=0, tiled=True)


def swap_cores(value):
    return lax.ppermute(value, "c", [(0, 1), (1, 0)])


def whole(shape, dtype):
    return pltpu.VMEM(shape, dtype)


def far(shape, dtype):
    return pltpu.HBM(shape, dtype)


def near(value):
    return pltpu.with_memory_space_constraint(value, pltpu.VMEM)


SCALARS = pl.BlockSpec(memory_space=pltpu.SMEM)
VECTORS = pl.BlockSpec(memory_space=pltpu.VMEM)
LIMIT = pltpu.CompilerParams(vmem_limit_bytes=24 * 1024 * 1024)


def translate_kernel(flags, own, other, matrices, out, info, translator, arrived):
    fetch = pltpu.make_async_copy(matrices, translator, arrived)
    fetch.start()
    low_core = flags[0] == 0
    keep = flags[1].astype(F32)
    lane = lax.broadcasted_iota(jnp.int32, (CAP, ROWS), 1).astype(F32)
    slot = lax.broadcasted_iota(jnp.int32, (CAP, ROWS), 0).astype(F32)
    base = jnp.zeros((1, 1), F32)
    pick_own, pick_other = [], []
    for k in range(8):
        count_own = own[k, INFO + 2 : INFO + 3, 0:1].astype(F32)
        count_other = other[k, INFO + 2 : INFO + 3, 0:1].astype(F32)
        start_own = base + jnp.where(low_core, 0.0, count_other)
        start_other = base + jnp.where(low_core, count_own, 0.0)
        hit_own = (lane == start_own + slot) & (slot < count_own)
        hit_other = (lane == start_other + slot) & (slot < count_other)
        pick_own.append(jnp.where(hit_own, 1.0, 0.0).astype(BF16))
        pick_other.append(jnp.where(hit_other, 1.0, 0.0).astype(BF16))
        base = base + count_own + count_other
        a = own[k, INFO : INFO + 8, 0:128].astype(F32)
        b = other[k, INFO : INFO + 8, 0:128].astype(F32)
        info[2 * k] = jnp.where(low_core, a, b)
        info[2 * k + 1] = jnp.where(low_core, b, a)
    pick_own = jnp.concatenate(pick_own, axis=0)
    pick_other = jnp.concatenate(pick_other, axis=0)
    fetch.wait()
    for layer in range(LAYERS + 1):
        low = layer * CAP
        a = own[:, low : low + CAP, :].reshape(ROWS, -1)
        b = other[:, low : low + CAP, :].reshape(ROWS, -1)
        rows = lax.dot_general(pick_own, a, TN, preferred_element_type=F32)
        rows = rows + lax.dot_general(pick_other, b, TN, preferred_element_type=F32)
        part = rows * keep
        if layer < LAYERS:
            part = part + dot(rows.astype(BF16), translator[layer])
        out[:, layer] = part.astype(BF16).reshape(16, 16, -1)


def high_low(value):
    high = value.astype(BF16).astype(F32)
    row = lax.broadcasted_iota(jnp.int32, value.shape, 0)
    return jnp.where(row == 0, high, jnp.where(row == 1, value - high, 0.0))


def scale_kernel(parts, bias, gain, y_out):
    x = parts[0].astype(F32)
    for k in range(1, 16):
        x = x + parts[k].astype(F32)
    x = x + bias[...]
    y = (x * gain[...]).astype(BF16)
    square = x * x
    square = jnp.concatenate([square] * 4, axis=0)
    ones = jnp.ones((8, x.shape[1]), F32)
    squares = lax.dot_general(ones, square, NT, precision=lax.Precision.HIGHEST, preferred_element_type=F32)
    squares = high_low(squares)
    for k in range(32):
        y_out[k, 0:64] = y
        y_out[k, 64:72] = jnp.zeros((8, x.shape[1]), BF16)
        y_out[k, 64:72, 0:256] = squares.astype(BF16)


def squares_of(y, chunk):
    lane = lax.broadcasted_iota(jnp.int32, (8, 256), 1)
    square = jnp.zeros((8, 256), F32)
    for j in range(4):
        total = jnp.zeros((1, 256), F32)
        for half in range(2):
            both = y[16 * half + 4 * chunk + j, 64:72, 0:256].astype(F32)
            total = total + both[0:1] + both[1:2]
        square = jnp.where(lane // 64 == j, jnp.broadcast_to(total, (8, 256)), square)
    return square


def own_kernel(flags, y, u_near, u_far, out):
    pair = flags[2]
    a = y[pl.ds(16 * pair, 16), 0:64, :].reshape(1024, -1)
    b = y[pl.ds(16 * (1 - pair), 16), 0:64, :].reshape(1024, -1)
    part = lax.dot_general(a, u_near[...], NT, preferred_element_type=F32)
    part = part + lax.dot_general(b, u_far[...], NT, preferred_element_type=F32)
    out[:, 0:256, :] = part.reshape(4, 256, -1)
    for k in range(4):
        out[k, 256:264, 0:256] = squares_of(y, k)


def chunk_kernel(step, flags, own_part, y_other, u_near, u_far, out):
    pair = flags[2]
    chunk = (flags[3] + step) % 4
    a = y_other[pl.ds(16 * pair + 4 * chunk, 4), 0:64, :].reshape(256, -1)
    b = y_other[pl.ds(16 * (1 - pair) + 4 * chunk, 4), 0:64, :].reshape(256, -1)
    part = lax.dot_general(a, u_near[...], NT, preferred_element_type=F32)
    part = part + lax.dot_general(b, u_far[...], NT, preferred_element_type=F32)
    out[0:256, :] = (own_part[chunk, 0:256, :] + part) * (1.0 / SHIFT)
    out[256:264, :] = jnp.zeros((8, out.shape[1]), F32)
    square = own_part[chunk, 256:264, 0:256] + squares_of(y_other, chunk)
    row = lax.broadcasted_iota(jnp.int32, square.shape, 0)
    large = square >= LARGE
    value = jnp.where(row < 2, jnp.where(large, square * (1.0 / SCALE), 0.0), jnp.where(large, 0.0, square))
    high = value.astype(BF16).astype(F32)
    value = jnp.where(row % 2 == 0, high, value - high)
    out[256:264, 0:256] = jnp.where(row < 4, value, 0.0)


def stats_kernel(summed, target, out):
    rows = summed[256:264, 0:256]
    square = (rows[0:1] + rows[1:2]) * SCALE + rows[2:3] + rows[3:4]
    factor = SHIFT * lax.rsqrt(square * (1.0 / D) + 1e-05)
    factor = jnp.broadcast_to(factor, (128, 256)).T[:, 0:1]
    logits = summed[0:256] * factor
    width = logits.shape[1]
    expz = jnp.exp(logits)
    total = jnp.sum(expz, axis=1, keepdims=True)
    ids = lax.broadcasted_iota(jnp.int32, logits.shape, 1)
    picked = jnp.sum(jnp.where(ids == target[...], logits, 0.0), axis=1, keepdims=True)
    four = logits.reshape(4, 4, 16, width)
    last = expz.reshape(4, 4, 16, width)[:, 3:]
    cross = jnp.sum(last * (four[:, 3:] - four), axis=3, keepdims=True).reshape(256, 1)
    lane = lax.broadcasted_iota(jnp.int32, (128, 128), 1)
    table = jnp.zeros((128, 128), F32)
    for h in range(2):
        for k, value in enumerate((total, cross, picked)):
            table = jnp.where(lane == 3 * h + k, value[128 * h : 128 * h + 128], table)
    rows = table.T[:8]
    for k in range(64):
        out[k] = rows


def body(
    probe_states,
    final_states,
    translator,
    translator_bias,
    norm_gain,
    unembed,
    answer_rows,
    answer_count,
    targets,
):
    zq = lax.axis_index("zq")
    c = lax.axis_index("c")
    quarter = 2 * lax.axis_index("zp") + c
    v = lax.axis_index(VOCAB)
    seq = 4 * zq + quarter
    width = probe_states.shape[2]
    part = unembed.shape[0] // 4
    picks = answer_rows[0]

    info = jnp.concatenate(
        [targets // 256, targets % 256, jnp.broadcast_to(answer_count[:, None], (1, CAP)), jnp.zeros((5, CAP), jnp.int32)]
    )
    info = jnp.pad(info, ((0, 0), (0, width - CAP))).astype(BF16)
    local = jnp.concatenate(
        [
            jnp.take(probe_states, picks, axis=1, mode="clip").reshape(LAYERS * CAP, width),
            jnp.take(final_states, picks, axis=0, mode="clip"),
            info,
        ],
        axis=0,
    )
    own = exchange(jnp.broadcast_to(local[None], (8, *local.shape)), Z)
    other = swap_cores(own)

    flags = jnp.stack([c, (seq == v).astype(jnp.int32), quarter // 2, zq])
    parts, every_info = pl.pallas_call(
        translate_kernel,
        out_shape=(far((16, 4, 16, width), BF16), far((16, 8, 128), F32)),
        in_specs=[SCALARS, VECTORS, VECTORS, pl.BlockSpec(memory_space=pltpu.HBM)],
        out_specs=(VECTORS, VECTORS),
        scratch_shapes=[pltpu.VMEM(translator.shape, BF16), pltpu.SemaphoreType.DMA(())],
        compiler_params=LIMIT,
        name="translate",
    )(flags, near(own), near(other), pltpu.with_memory_space_constraint(translator, pltpu.HBM))
    arrived = exchange(parts.reshape(16, 64, width), VOCAB)
    fours = unembed.reshape(4, part, width)
    quarters = []
    for k in range(4):
        block = lax.dynamic_index_in_dim(fours, quarter ^ k, 0, keepdims=False)
        if k:
            block = lax.ppermute(block, ("zp", "c"), [(j, j ^ k) for j in range(4)])
        quarters.append(block)

    bias = jnp.concatenate([translator_bias, jnp.zeros((1, width), F32)], axis=0)
    bias = jnp.repeat(bias, 16, axis=0)
    y_copies = pl.pallas_call(
        scale_kernel,
        out_shape=whole((32, 72, width), BF16),
        in_specs=[VECTORS] * 3,
        out_specs=VECTORS,
        compiler_params=LIMIT,
        name="scale",
    )(near(arrived), bias, norm_gain[None, :])
    y_own = exchange(y_copies, ("zp", *VOCAB))
    y_other = swap_cores(y_own)

    quarters = [near(block) for block in quarters]
    y_own, y_other = near(y_own), near(y_other)
    own_part = pl.pallas_call(
        own_kernel,
        out_shape=whole((4, 264, part), F32),
        in_specs=[SCALARS] + [VECTORS] * 3,
        out_specs=VECTORS,
        compiler_params=LIMIT,
        name="own_logits",
    )(flags, y_own, quarters[0], quarters[2])
    chunks = []
    for k in (2, 1, 3, 0):
        chunk = pl.pallas_call(
            functools.partial(chunk_kernel, k),
            out_shape=whole((264, part), F32),
            in_specs=[SCALARS] + [VECTORS] * 4,
            out_specs=VECTORS,
            compiler_params=LIMIT,
        )(flags, near(own_part), y_other, quarters[1], quarters[3])
        if k:
            chunk = chunk.astype(jnp.float16)
            chunk = lax.ppermute(chunk, "zq", [(j, (j + k) % 4) for j in range(4)])
        else:
            every_info, chunk = lax.optimization_barrier((every_info, chunk))
        chunks.append(chunk)
    summed = chunks[3]
    for chunk in chunks[:3]:
        summed = summed + chunk.astype(F32)

    every_info = every_info[:, :3, :CAP].astype(jnp.int32)
    counts = every_info[:, 2, 0]
    all_targets = every_info[:, 0] * 256 + every_info[:, 1]
    order = jnp.arange(16, dtype=jnp.int32)
    starts = jnp.sum(jnp.where(order[None, :] < order[:, None], counts[None, :], 0), axis=1)
    slots = jnp.arange(CAP, dtype=jnp.int32)
    place = jnp.where(slots[None, :] < counts[:, None], starts[:, None] + slots[None, :], -1)
    row_ids = zq * 64 + jnp.arange(64, dtype=jnp.int32)
    hit = place[None] == row_ids[:, None, None]
    row_targets = jnp.sum(jnp.where(hit, all_targets[None], 0), axis=(1, 2))
    local_targets = row_targets - (v * 4 + quarter) * part
    item_targets = jnp.broadcast_to(local_targets.reshape(4, 1, 16), (4, 4, 16)).reshape(256, 1)
    stats = pl.pallas_call(
        stats_kernel,
        out_shape=far((64, 8, 128), F32),
        in_specs=[VECTORS] * 2,
        out_specs=VECTORS,
        compiler_params=LIMIT,
        name="stats",
    )(near(summed), item_targets)
    sums = jnp.sum(exchange(stats, ("zp", "c", *VOCAB)), axis=0)
    every = [sums]
    for k in (1, 2, 3):
        every.append(lax.ppermute(sums, "zq", [(j, (j + k) % 4) for j in range(4)]))
    every = jnp.stack(every)

    table = every[:, :6].reshape(4, 2, 3, 2, 4, 16).transpose(2, 4, 0, 1, 3, 5).reshape(3, 4, 1, ROWS)
    chunk = (zq - jnp.arange(4, dtype=jnp.int32)) % 4
    held = (chunk[:, None] * 64 + jnp.arange(64, dtype=jnp.int32)[None, :]).reshape(1, ROWS)
    my_start = jnp.sum(jnp.where(order == seq, starts, 0))
    live = slots < answer_count[0]
    wanted = my_start + slots
    mine = wanted[:, None] == held
    mine = jnp.sum(jnp.where(mine[None, None], table, 0.0), axis=3)
    log_total = jnp.log(mine[0])
    logprob = mine[2] - log_total
    divergence = mine[1, :LAYERS] / mine[0, LAYERS:] - log_total[LAYERS:] + log_total[:LAYERS]
    logprob = jnp.where(live[None], logprob, 0.0)[:, None, :]
    divergence = jnp.where(live[None], divergence, 0.0)[:, None, :]
    return (logprob, divergence)


def solution(mesh):
    split = Mesh(mesh.devices.reshape(4, 2, 2, 4, 4), ("zq", "zp", "c", "y", "x"))
    return jax.shard_map(
        body,
        mesh=split,
        in_specs=(
            P(None, SEQ, VOCAB),
            P(SEQ, VOCAB),
            P(None, VOCAB, SEQ),
            P(None, SEQ),
            P(SEQ),
            P(VOCAB, SEQ),
            P(SEQ, None),
            P(SEQ),
            P(SEQ, None),
        ),
        out_specs=(P(None, SEQ, None), P(None, SEQ, None)),
        check_vma=False,
    )
```

```python
import functools

import jax
import jax.numpy as jnp
from jax import lax
from jax.experimental import pallas as pl
from jax.experimental.pallas import tpu as pltpu
from jax.sharding import Mesh
from jax.sharding import PartitionSpec as P


D = 6144
LAYERS = 3
CAP = 32
ROWS = 256
Z = ("zq", "zp")
SEQ = ("zq", "zp", "c")
VOCAB = ("y", "x")
F32 = jnp.float32
BF16 = jnp.bfloat16
NT = (((1,), (1,)), ((), ()))
TN = (((0,), (0,)), ((), ()))
INFO = 128
OFFSETS = (0, -2, 2, -1, 1, -3, 3, -4)
SHIFT = 16.0
SCALE = 262144.0
LARGE = 16.0


def dot(a, b):
    return jnp.dot(a, b, preferred_element_type=F32)


def exchange(value, axes):
    return lax.all_to_all(value, axes, split_axis=0, concat_axis=0, tiled=True)


def shifted(value, by):
    return lax.ppermute(value, Z, [(j, (j + by) % 8) for j in range(8)])


def swap_cores(value):
    return lax.ppermute(value, "c", [(0, 1), (1, 0)])


def whole(shape, dtype):
    return pltpu.VMEM(shape, dtype)


def far(shape, dtype):
    return pltpu.HBM(shape, dtype)


def near(value):
    return pltpu.with_memory_space_constraint(value, pltpu.VMEM)


SCALARS = pl.BlockSpec(memory_space=pltpu.SMEM)
VECTORS = pl.BlockSpec(memory_space=pltpu.VMEM)
LIMIT = pltpu.CompilerParams(vmem_limit_bytes=24 * 1024 * 1024)


def translate_kernel(flags, *refs):
    own, other = refs[:8], refs[8:16]
    translator, out, info = refs[16:]
    low_core = flags[0] == 0
    keep = flags[1].astype(F32)
    chips = [lax.rem(flags[4] + offset + 8, 8) for offset in OFFSETS]
    lane = lax.broadcasted_iota(jnp.int32, (CAP, ROWS), 1).astype(F32)
    slot = lax.broadcasted_iota(jnp.int32, (CAP, ROWS), 0).astype(F32)
    counts_own = [ref[INFO + 2 : INFO + 3, 0:1].astype(F32) for ref in own]
    counts_other = [ref[INFO + 2 : INFO + 3, 0:1].astype(F32) for ref in other]
    pick_own, pick_other = [], []
    for k in range(8):
        base = jnp.zeros((1, 1), F32)
        for j in range(8):
            if j != k:
                base = base + jnp.where(chips[j] < chips[k], counts_own[j] + counts_other[j], 0.0)
        start_own = base + jnp.where(low_core, 0.0, counts_other[k])
        start_other = base + jnp.where(low_core, counts_own[k], 0.0)
        hit_own = (lane == start_own + slot) & (slot < counts_own[k])
        hit_other = (lane == start_other + slot) & (slot < counts_other[k])
        pick_own.append(jnp.where(hit_own, 1.0, 0.0).astype(BF16))
        pick_other.append(jnp.where(hit_other, 1.0, 0.0).astype(BF16))
        a = own[k][INFO : INFO + 8, 0:128].astype(F32)
        b = other[k][INFO : INFO + 8, 0:128].astype(F32)
        info[2 * chips[k]] = jnp.where(low_core, a, b)
        info[2 * chips[k] + 1] = jnp.where(low_core, b, a)
    pick_own = jnp.concatenate(pick_own, axis=0)
    pick_other = jnp.concatenate(pick_other, axis=0)
    for layer in range(LAYERS + 1):
        low = layer * CAP
        a = jnp.concatenate([ref[low : low + CAP, :] for ref in own], axis=0)
        b = jnp.concatenate([ref[low : low + CAP, :] for ref in other], axis=0)
        rows = lax.dot_general(pick_own, a, TN, preferred_element_type=F32)
        rows = rows + lax.dot_general(pick_other, b, TN, preferred_element_type=F32)
        part = rows * keep
        if layer < LAYERS:
            part = part + dot(rows.astype(BF16), translator[layer])
        out[:, layer] = part.astype(BF16).reshape(16, 16, -1)


def high_low(value):
    high = value.astype(BF16).astype(F32)
    row = lax.broadcasted_iota(jnp.int32, value.shape, 0)
    return jnp.where(row == 0, high, jnp.where(row == 1, value - high, 0.0))


def scale_kernel(parts, bias, gain, y_out):
    x = parts[0].astype(F32)
    for k in range(1, 16):
        x = x + parts[k].astype(F32)
    x = x + bias[...]
    y = (x * gain[...]).astype(BF16)
    square = x * x
    square = jnp.concatenate([square] * 4, axis=0)
    ones = jnp.ones((8, x.shape[1]), F32)
    squares = lax.dot_general(ones, square, NT, precision=lax.Precision.HIGHEST, preferred_element_type=F32)
    squares = high_low(squares)
    for k in range(32):
        y_out[k, 0:64] = y
        y_out[k, 64:72] = jnp.zeros((8, x.shape[1]), BF16)
        y_out[k, 64:72, 0:256] = squares.astype(BF16)


def squares_of(y, chunk):
    lane = lax.broadcasted_iota(jnp.int32, (8, 256), 1)
    square = jnp.zeros((8, 256), F32)
    for j in range(4):
        total = jnp.zeros((1, 256), F32)
        for half in range(2):
            both = y[16 * half + 4 * chunk + j, 64:72, 0:256].astype(F32)
            total = total + both[0:1] + both[1:2]
        square = jnp.where(lane // 64 == j, jnp.broadcast_to(total, (8, 256)), square)
    return square


def own_kernel(flags, y, u_near, u_far, out):
    pair = flags[2]
    a = y[pl.ds(16 * pair, 16), 0:64, :].reshape(1024, -1)
    b = y[pl.ds(16 * (1 - pair), 16), 0:64, :].reshape(1024, -1)
    part = lax.dot_general(a, u_near[...], NT, preferred_element_type=F32)
    part = part + lax.dot_general(b, u_far[...], NT, preferred_element_type=F32)
    out[:, 0:256, :] = part.reshape(4, 256, -1)
    for k in range(4):
        out[k, 256:264, 0:256] = squares_of(y, k)


def chunk_kernel(step, flags, own_part, y_other, u_near, u_far, out):
    pair = flags[2]
    chunk = (flags[3] + step) % 4
    a = y_other[pl.ds(16 * pair + 4 * chunk, 4), 0:64, :].reshape(256, -1)
    b = y_other[pl.ds(16 * (1 - pair) + 4 * chunk, 4), 0:64, :].reshape(256, -1)
    part = lax.dot_general(a, u_near[...], NT, preferred_element_type=F32)
    part = part + lax.dot_general(b, u_far[...], NT, preferred_element_type=F32)
    out[0:256, :] = (own_part[chunk, 0:256, :] + part) * (1.0 / SHIFT)
    out[256:264, :] = jnp.zeros((8, out.shape[1]), F32)
    square = own_part[chunk, 256:264, 0:256] + squares_of(y_other, chunk)
    row = lax.broadcasted_iota(jnp.int32, square.shape, 0)
    large = square >= LARGE
    value = jnp.where(row < 2, jnp.where(large, square * (1.0 / SCALE), 0.0), jnp.where(large, 0.0, square))
    high = value.astype(BF16).astype(F32)
    value = jnp.where(row % 2 == 0, high, value - high)
    out[256:264, 0:256] = jnp.where(row < 4, value, 0.0)


def stats_kernel(summed, target, out):
    rows = summed[256:264, 0:256]
    square = (rows[0:1] + rows[1:2]) * SCALE + rows[2:3] + rows[3:4]
    factor = SHIFT * lax.rsqrt(square * (1.0 / D) + 1e-05)
    factor = jnp.broadcast_to(factor, (128, 256)).T[:, 0:1]
    logits = summed[0:256] * factor
    width = logits.shape[1]
    expz = jnp.exp(logits)
    total = jnp.sum(expz, axis=1, keepdims=True)
    ids = lax.broadcasted_iota(jnp.int32, logits.shape, 1)
    picked = jnp.sum(jnp.where(ids == target[...], logits, 0.0), axis=1, keepdims=True)
    four = logits.reshape(4, 4, 16, width)
    last = expz.reshape(4, 4, 16, width)[:, 3:]
    cross = jnp.sum(last * (four[:, 3:] - four), axis=3, keepdims=True).reshape(256, 1)
    lane = lax.broadcasted_iota(jnp.int32, (128, 128), 1)
    table = jnp.zeros((128, 128), F32)
    for h in range(2):
        for k, value in enumerate((total, cross, picked)):
            table = jnp.where(lane == 3 * h + k, value[128 * h : 128 * h + 128], table)
    rows = table.T[:8]
    for k in range(64):
        out[k] = rows


def body(
    probe_states,
    final_states,
    translator,
    translator_bias,
    norm_gain,
    unembed,
    answer_rows,
    answer_count,
    targets,
):
    zq = lax.axis_index("zq")
    c = lax.axis_index("c")
    quarter = 2 * lax.axis_index("zp") + c
    v = lax.axis_index(VOCAB)
    seq = 4 * zq + quarter
    width = probe_states.shape[2]
    part = unembed.shape[0] // 4
    picks = answer_rows[0]

    info = jnp.concatenate(
        [targets // 256, targets % 256, jnp.broadcast_to(answer_count[:, None], (1, CAP)), jnp.zeros((5, CAP), jnp.int32)]
    )
    info = jnp.pad(info, ((0, 0), (0, width - CAP))).astype(BF16)
    local = jnp.concatenate(
        [
            jnp.take(probe_states, picks, axis=1, mode="clip").reshape(LAYERS * CAP, width),
            jnp.take(final_states, picks, axis=0, mode="clip"),
            info,
        ],
        axis=0,
    )
    back2, fore2, back1, fore1 = [shifted(local, by) for by in (2, -2, 1, -1)]
    own = [local, back2, fore2, back1, fore1]
    other = [swap_cores(chunk) for chunk in own]
    third = [shifted(back2, 1), shifted(fore2, -1), shifted(back2, 2)]
    own += third
    other += [swap_cores(chunk) for chunk in third]

    flags = jnp.stack([c, (seq == v).astype(jnp.int32), quarter // 2, zq, seq // 2])
    parts, every_info = pl.pallas_call(
        translate_kernel,
        out_shape=(far((16, 4, 16, width), BF16), far((16, 8, 128), F32)),
        in_specs=[SCALARS] + [VECTORS] * 17,
        out_specs=(VECTORS, VECTORS),
        compiler_params=LIMIT,
        name="translate",
    )(flags, *[near(chunk) for chunk in own + other], near(translator))
    arrived = exchange(parts.reshape(16, 64, width), VOCAB)
    fours = unembed.reshape(4, part, width)
    quarters = []
    for k in range(4):
        block = lax.dynamic_index_in_dim(fours, quarter ^ k, 0, keepdims=False)
        if k:
            block = lax.ppermute(block, ("zp", "c"), [(j, j ^ k) for j in range(4)])
        quarters.append(block)

    bias = jnp.concatenate([translator_bias, jnp.zeros((1, width), F32)], axis=0)
    bias = jnp.repeat(bias, 16, axis=0)
    y_copies = pl.pallas_call(
        scale_kernel,
        out_shape=whole((32, 72, width), BF16),
        in_specs=[VECTORS] * 3,
        out_specs=VECTORS,
        compiler_params=LIMIT,
        name="scale",
    )(near(arrived), bias, norm_gain[None, :])
    y_own = exchange(y_copies, ("zp", *VOCAB))
    y_other = swap_cores(y_own)

    quarters = [near(block) for block in quarters]
    y_own, y_other = near(y_own), near(y_other)
    own_part = pl.pallas_call(
        own_kernel,
        out_shape=whole((4, 264, part), F32),
        in_specs=[SCALARS] + [VECTORS] * 3,
        out_specs=VECTORS,
        compiler_params=LIMIT,
        name="own_logits",
    )(flags, y_own, quarters[0], quarters[2])
    chunks = []
    for k in (2, 1, 3, 0):
        chunk = pl.pallas_call(
            functools.partial(chunk_kernel, k),
            out_shape=whole((264, part), F32),
            in_specs=[SCALARS] + [VECTORS] * 4,
            out_specs=VECTORS,
            compiler_params=LIMIT,
        )(flags, near(own_part), y_other, quarters[1], quarters[3])
        if k:
            chunk = chunk.astype(jnp.float16)
            chunk = lax.ppermute(chunk, "zq", [(j, (j + k) % 4) for j in range(4)])
        else:
            every_info, chunk = lax.optimization_barrier((every_info, chunk))
        chunks.append(chunk)
    summed = chunks[3]
    for chunk in chunks[:3]:
        summed = summed + chunk.astype(F32)

    every_info = every_info[:, :3, :CAP].astype(jnp.int32)
    counts = every_info[:, 2, 0]
    all_targets = every_info[:, 0] * 256 + every_info[:, 1]
    order = jnp.arange(16, dtype=jnp.int32)
    starts = jnp.sum(jnp.where(order[None, :] < order[:, None], counts[None, :], 0), axis=1)
    slots = jnp.arange(CAP, dtype=jnp.int32)
    place = jnp.where(slots[None, :] < counts[:, None], starts[:, None] + slots[None, :], -1)
    row_ids = zq * 64 + jnp.arange(64, dtype=jnp.int32)
    hit = place[None] == row_ids[:, None, None]
    row_targets = jnp.sum(jnp.where(hit, all_targets[None], 0), axis=(1, 2))
    local_targets = row_targets - (v * 4 + quarter) * part
    item_targets = jnp.broadcast_to(local_targets.reshape(4, 1, 16), (4, 4, 16)).reshape(256, 1)
    stats = pl.pallas_call(
        stats_kernel,
        out_shape=far((64, 8, 128), F32),
        in_specs=[VECTORS] * 2,
        out_specs=VECTORS,
        compiler_params=LIMIT,
        name="stats",
    )(near(summed), item_targets)
    sums = jnp.sum(exchange(stats, ("zp", "c", *VOCAB)), axis=0)
    every = [sums]
    for k in (1, 2, 3):
        every.append(lax.ppermute(sums, "zq", [(j, (j + k) % 4) for j in range(4)]))
    every = jnp.stack(every)

    table = every[:, :6].reshape(4, 2, 3, 2, 4, 16).transpose(2, 4, 0, 1, 3, 5).reshape(3, 4, 1, ROWS)
    chunk = (zq - jnp.arange(4, dtype=jnp.int32)) % 4
    held = (chunk[:, None] * 64 + jnp.arange(64, dtype=jnp.int32)[None, :]).reshape(1, ROWS)
    my_start = jnp.sum(jnp.where(order == seq, starts, 0))
    live = slots < answer_count[0]
    wanted = my_start + slots
    mine = wanted[:, None] == held
    mine = jnp.sum(jnp.where(mine[None, None], table, 0.0), axis=3)
    log_total = jnp.log(mine[0])
    logprob = mine[2] - log_total
    divergence = mine[1, :LAYERS] / mine[0, LAYERS:] - log_total[LAYERS:] + log_total[:LAYERS]
    logprob = jnp.where(live[None], logprob, 0.0)[:, None, :]
    divergence = jnp.where(live[None], divergence, 0.0)[:, None, :]
    return (logprob, divergence)


def solution(mesh):
    split = Mesh(mesh.devices.reshape(4, 2, 2, 4, 4), ("zq", "zp", "c", "y", "x"))
    return jax.shard_map(
        body,
        mesh=split,
        in_specs=(
            P(None, SEQ, VOCAB),
            P(SEQ, VOCAB),
            P(None, VOCAB, SEQ),
            P(None, SEQ),
            P(SEQ),
            P(VOCAB, SEQ),
            P(SEQ, None),
            P(SEQ),
            P(SEQ, None),
        ),
        out_specs=(P(None, SEQ, None), P(None, SEQ, None)),
        check_vma=False,
    )
```

```python
import functools

import jax
import jax.numpy as jnp
from jax import lax
from jax.experimental import pallas as pl
from jax.experimental.pallas import tpu as pltpu
from jax.sharding import Mesh
from jax.sharding import PartitionSpec as P


D = 6144
LAYERS = 3
CAP = 32
ROWS = 256
Z = ("zq", "zp")
SEQ = ("zq", "zp", "c")
VOCAB = ("y", "x")
F32 = jnp.float32
BF16 = jnp.bfloat16
NT = (((1,), (1,)), ((), ()))
TN = (((0,), (0,)), ((), ()))
INFO = 128
OFFSETS = (0, -2, 2, -1, 1, -3, 3, -4)
SHIFT = 16.0
SCALE = 262144.0
LARGE = 16.0


def dot(a, b):
    return jnp.dot(a, b, preferred_element_type=F32)


def exchange(value, axes):
    return lax.all_to_all(value, axes, split_axis=0, concat_axis=0, tiled=True)


def shifted(value, by):
    return lax.ppermute(value, Z, [(j, (j + by) % 8) for j in range(8)])


def swap_cores(value):
    return lax.ppermute(value, "c", [(0, 1), (1, 0)])


def whole(shape, dtype):
    return pltpu.VMEM(shape, dtype)


def far(shape, dtype):
    return pltpu.HBM(shape, dtype)


def near(value):
    return pltpu.with_memory_space_constraint(value, pltpu.VMEM)


def held(value):
    return pltpu.with_memory_space_constraint(value, pltpu.HBM)


SCALARS = pl.BlockSpec(memory_space=pltpu.SMEM)
VECTORS = pl.BlockSpec(memory_space=pltpu.VMEM)
LIMIT = pltpu.CompilerParams(vmem_limit_bytes=24 * 1024 * 1024)


def pick_kernel(picks, count, targets, probe, final_far, out, rows, final, arrived):
    fetch = pltpu.make_async_copy(final_far, final, arrived)
    fetch.start()
    sub = lax.broadcasted_iota(jnp.int32, (16, out.shape[1]), 0)

    def take(layer, k):
        pick = jnp.clip(picks[0, k], 0, final.shape[0] - 1)
        within = lax.rem(pick, 16)
        group = pl.ds(pl.multiple_of(pick - within, 16), 16)
        block = probe[layer, group, :] if layer < LAYERS else final[group, :]
        row = jnp.sum(jnp.where(sub == within, block.astype(F32), 0.0), axis=0, keepdims=True)
        rows[layer * CAP + k : layer * CAP + k + 1, :] = row

    for k in range(CAP):
        for layer in range(LAYERS):
            take(layer, k)
    fetch.wait()
    for k in range(CAP):
        take(LAYERS, k)
    out[0:INFO] = rows[...].astype(BF16)
    out[INFO : INFO + 8] = jnp.zeros((8, out.shape[1]), BF16)
    line = lax.broadcasted_iota(jnp.int32, (8, CAP), 0)
    wanted = jnp.broadcast_to(targets[...], (8, CAP))
    value = jnp.where(line == 0, wanted >> 8, jnp.where(line == 1, wanted & 255, jnp.where(line == 2, count[0], 0)))
    out[INFO : INFO + 8, 0:CAP] = value.astype(F32).astype(BF16)


def translate_kernel(flags, *refs):
    own, other = refs[:8], refs[8:16]
    translator, out, info = refs[16:]
    low_core = flags[0] == 0
    keep = flags[1].astype(F32)
    chips = [lax.rem(flags[4] + offset + 8, 8) for offset in OFFSETS]
    lane = lax.broadcasted_iota(jnp.int32, (CAP, ROWS), 1).astype(F32)
    slot = lax.broadcasted_iota(jnp.int32, (CAP, ROWS), 0).astype(F32)
    counts_own = [ref[INFO + 2 : INFO + 3, 0:1].astype(F32) for ref in own]
    counts_other = [ref[INFO + 2 : INFO + 3, 0:1].astype(F32) for ref in other]
    pick_own, pick_other = [], []
    for k in range(8):
        base = jnp.zeros((1, 1), F32)
        for j in range(8):
            if j != k:
                base = base + jnp.where(chips[j] < chips[k], counts_own[j] + counts_other[j], 0.0)
        start_own = base + jnp.where(low_core, 0.0, counts_other[k])
        start_other = base + jnp.where(low_core, counts_own[k], 0.0)
        hit_own = (lane == start_own + slot) & (slot < counts_own[k])
        hit_other = (lane == start_other + slot) & (slot < counts_other[k])
        pick_own.append(jnp.where(hit_own, 1.0, 0.0).astype(BF16))
        pick_other.append(jnp.where(hit_other, 1.0, 0.0).astype(BF16))
        a = own[k][INFO : INFO + 8, 0:128].astype(F32)
        b = other[k][INFO : INFO + 8, 0:128].astype(F32)
        info[2 * chips[k]] = jnp.where(low_core, a, b)
        info[2 * chips[k] + 1] = jnp.where(low_core, b, a)
    pick_own = jnp.concatenate(pick_own, axis=0)
    pick_other = jnp.concatenate(pick_other, axis=0)
    for layer in range(LAYERS + 1):
        low = layer * CAP
        a = jnp.concatenate([ref[low : low + CAP, :] for ref in own], axis=0)
        b = jnp.concatenate([ref[low : low + CAP, :] for ref in other], axis=0)
        rows = lax.dot_general(pick_own, a, TN, preferred_element_type=F32)
        rows = rows + lax.dot_general(pick_other, b, TN, preferred_element_type=F32)
        part = rows * keep
        if layer < LAYERS:
            part = part + dot(rows.astype(BF16), translator[layer])
        out[:, layer] = part.astype(BF16).reshape(16, 16, -1)


def high_low(value):
    high = value.astype(BF16).astype(F32)
    row = lax.broadcasted_iota(jnp.int32, value.shape, 0)
    return jnp.where(row == 0, high, jnp.where(row == 1, value - high, 0.0))


def scale_kernel(parts, bias, gain, y_out):
    x = parts[0].astype(F32)
    for k in range(1, 16):
        x = x + parts[k].astype(F32)
    x = x + bias[...]
    y = (x * gain[...]).astype(BF16)
    square = x * x
    square = jnp.concatenate([square] * 4, axis=0)
    ones = jnp.ones((8, x.shape[1]), F32)
    squares = lax.dot_general(ones, square, NT, precision=lax.Precision.HIGHEST, preferred_element_type=F32)
    squares = high_low(squares)
    for k in range(32):
        y_out[k, 0:64] = y
        y_out[k, 64:72] = jnp.zeros((8, x.shape[1]), BF16)
        y_out[k, 64:72, 0:256] = squares.astype(BF16)


def squares_of(y, chunk):
    lane = lax.broadcasted_iota(jnp.int32, (8, 256), 1)
    square = jnp.zeros((8, 256), F32)
    for j in range(4):
        total = jnp.zeros((1, 256), F32)
        for half in range(2):
            both = y[16 * half + 4 * chunk + j, 64:72, 0:256].astype(F32)
            total = total + both[0:1] + both[1:2]
        square = jnp.where(lane // 64 == j, jnp.broadcast_to(total, (8, 256)), square)
    return square


def own_kernel(flags, y, u_near, u_far, out):
    pair = flags[2]
    a = y[pl.ds(16 * pair, 16), 0:64, :].reshape(1024, -1)
    b = y[pl.ds(16 * (1 - pair), 16), 0:64, :].reshape(1024, -1)
    part = lax.dot_general(a, u_near[...], NT, preferred_element_type=F32)
    part = part + lax.dot_general(b, u_far[...], NT, preferred_element_type=F32)
    out[:, 0:256, :] = part.reshape(4, 256, -1)
    for k in range(4):
        out[k, 256:264, 0:256] = squares_of(y, k)


def chunk_kernel(step, flags, own_part, y_other, u_near, u_far, out):
    pair = flags[2]
    chunk = (flags[3] + step) % 4
    a = y_other[pl.ds(16 * pair + 4 * chunk, 4), 0:64, :].reshape(256, -1)
    b = y_other[pl.ds(16 * (1 - pair) + 4 * chunk, 4), 0:64, :].reshape(256, -1)
    part = lax.dot_general(a, u_near[...], NT, preferred_element_type=F32)
    part = part + lax.dot_general(b, u_far[...], NT, preferred_element_type=F32)
    out[0:256, :] = (own_part[chunk, 0:256, :] + part) * (1.0 / SHIFT)
    out[256:264, :] = jnp.zeros((8, out.shape[1]), F32)
    square = own_part[chunk, 256:264, 0:256] + squares_of(y_other, chunk)
    row = lax.broadcasted_iota(jnp.int32, square.shape, 0)
    large = square >= LARGE
    value = jnp.where(row < 2, jnp.where(large, square * (1.0 / SCALE), 0.0), jnp.where(large, 0.0, square))
    high = value.astype(BF16).astype(F32)
    value = jnp.where(row % 2 == 0, high, value - high)
    out[256:264, 0:256] = jnp.where(row < 4, value, 0.0)


def stats_kernel(summed, target, out):
    rows = summed[256:264, 0:256]
    square = (rows[0:1] + rows[1:2]) * SCALE + rows[2:3] + rows[3:4]
    factor = SHIFT * lax.rsqrt(square * (1.0 / D) + 1e-05)
    factor = jnp.broadcast_to(factor, (128, 256)).T[:, 0:1]
    logits = summed[0:256] * factor
    width = logits.shape[1]
    expz = jnp.exp(logits)
    total = jnp.sum(expz, axis=1, keepdims=True)
    ids = lax.broadcasted_iota(jnp.int32, logits.shape, 1)
    picked = jnp.sum(jnp.where(ids == target[...], logits, 0.0), axis=1, keepdims=True)
    four = logits.reshape(4, 4, 16, width)
    last = expz.reshape(4, 4, 16, width)[:, 3:]
    cross = jnp.sum(last * (four[:, 3:] - four), axis=3, keepdims=True).reshape(256, 1)
    lane = lax.broadcasted_iota(jnp.int32, (128, 128), 1)
    table = jnp.zeros((128, 128), F32)
    for h in range(2):
        for k, value in enumerate((total, cross, picked)):
            table = jnp.where(lane == 3 * h + k, value[128 * h : 128 * h + 128], table)
    rows = table.T[:8]
    for k in range(64):
        out[k] = rows


def body(
    probe_states,
    final_states,
    translator,
    translator_bias,
    norm_gain,
    unembed,
    answer_rows,
    answer_count,
    targets,
):
    zq = lax.axis_index("zq")
    c = lax.axis_index("c")
    quarter = 2 * lax.axis_index("zp") + c
    v = lax.axis_index(VOCAB)
    seq = 4 * zq + quarter
    width = probe_states.shape[2]
    part = unembed.shape[0] // 4

    local = pl.pallas_call(
        pick_kernel,
        out_shape=whole((INFO + 8, width), BF16),
        in_specs=[SCALARS] * 2 + [VECTORS] * 2 + [pl.BlockSpec(memory_space=pltpu.HBM)],
        out_specs=VECTORS,
        scratch_shapes=[
            pltpu.VMEM((INFO, width), F32),
            pltpu.VMEM(final_states.shape, BF16),
            pltpu.SemaphoreType.DMA(()),
        ],
        compiler_params=LIMIT,
        name="pick",
    )(answer_rows, answer_count, held(targets), near(probe_states), held(final_states))
    back2, fore2, back1, fore1 = [shifted(local, by) for by in (2, -2, 1, -1)]
    own = [local, back2, fore2, back1, fore1]
    other = [swap_cores(chunk) for chunk in own]
    third = [shifted(back2, 1), shifted(fore2, -1), shifted(back2, 2)]
    own += third
    other += [swap_cores(chunk) for chunk in third]

    flags = jnp.stack([c, (seq == v).astype(jnp.int32), quarter // 2, zq, seq // 2])
    parts, every_info = pl.pallas_call(
        translate_kernel,
        out_shape=(far((16, 4, 16, width), BF16), far((16, 8, 128), F32)),
        in_specs=[SCALARS] + [VECTORS] * 17,
        out_specs=(VECTORS, VECTORS),
        compiler_params=LIMIT,
        name="translate",
    )(flags, *[near(chunk) for chunk in own + other], near(translator))
    arrived = exchange(parts.reshape(16, 64, width), VOCAB)
    fours = unembed.reshape(4, part, width)
    quarters = []
    for k in range(4):
        block = lax.dynamic_index_in_dim(fours, quarter ^ k, 0, keepdims=False)
        if k:
            block = lax.ppermute(block, ("zp", "c"), [(j, j ^ k) for j in range(4)])
        quarters.append(block)

    bias = jnp.concatenate([translator_bias, jnp.zeros((1, width), F32)], axis=0)
    bias = jnp.repeat(bias, 16, axis=0)
    y_copies = pl.pallas_call(
        scale_kernel,
        out_shape=whole((32, 72, width), BF16),
        in_specs=[VECTORS] * 3,
        out_specs=VECTORS,
        compiler_params=LIMIT,
        name="scale",
    )(near(arrived), bias, norm_gain[None, :])
    y_own = exchange(y_copies, ("zp", *VOCAB))
    y_other = swap_cores(y_own)

    quarters = [near(block) for block in quarters]
    y_own, y_other = near(y_own), near(y_other)
    own_part = pl.pallas_call(
        own_kernel,
        out_shape=whole((4, 264, part), F32),
        in_specs=[SCALARS] + [VECTORS] * 3,
        out_specs=VECTORS,
        compiler_params=LIMIT,
        name="own_logits",
    )(flags, y_own, quarters[0], quarters[2])
    chunks = []
    for k in (2, 1, 3, 0):
        chunk = pl.pallas_call(
            functools.partial(chunk_kernel, k),
            out_shape=whole((264, part), F32),
            in_specs=[SCALARS] + [VECTORS] * 4,
            out_specs=VECTORS,
            compiler_params=LIMIT,
        )(flags, near(own_part), y_other, quarters[1], quarters[3])
        if k:
            chunk = chunk.astype(jnp.float16)
            chunk = lax.ppermute(chunk, "zq", [(j, (j + k) % 4) for j in range(4)])
        else:
            every_info, chunk = lax.optimization_barrier((every_info, chunk))
        chunks.append(chunk)
    summed = chunks[3]
    for chunk in chunks[:3]:
        summed = summed + chunk.astype(F32)

    every_info = every_info[:, :3, :CAP].astype(jnp.int32)
    counts = every_info[:, 2, 0]
    all_targets = every_info[:, 0] * 256 + every_info[:, 1]
    order = jnp.arange(16, dtype=jnp.int32)
    starts = jnp.sum(jnp.where(order[None, :] < order[:, None], counts[None, :], 0), axis=1)
    slots = jnp.arange(CAP, dtype=jnp.int32)
    place = jnp.where(slots[None, :] < counts[:, None], starts[:, None] + slots[None, :], -1)
    row_ids = zq * 64 + jnp.arange(64, dtype=jnp.int32)
    hit = place[None] == row_ids[:, None, None]
    row_targets = jnp.sum(jnp.where(hit, all_targets[None], 0), axis=(1, 2))
    local_targets = row_targets - (v * 4 + quarter) * part
    item_targets = jnp.broadcast_to(local_targets.reshape(4, 1, 16), (4, 4, 16)).reshape(256, 1)
    stats = pl.pallas_call(
        stats_kernel,
        out_shape=far((64, 8, 128), F32),
        in_specs=[VECTORS] * 2,
        out_specs=VECTORS,
        compiler_params=LIMIT,
        name="stats",
    )(near(summed), item_targets)
    sums = jnp.sum(exchange(stats, ("zp", "c", *VOCAB)), axis=0)
    every = [sums]
    for k in (1, 2, 3):
        every.append(lax.ppermute(sums, "zq", [(j, (j + k) % 4) for j in range(4)]))
    every = jnp.stack(every)

    table = every[:, :6].reshape(4, 2, 3, 2, 4, 16).transpose(2, 4, 0, 1, 3, 5).reshape(3, 4, 1, ROWS)
    chunk = (zq - jnp.arange(4, dtype=jnp.int32)) % 4
    ids = (chunk[:, None] * 64 + jnp.arange(64, dtype=jnp.int32)[None, :]).reshape(1, ROWS)
    my_start = jnp.sum(jnp.where(order == seq, starts, 0))
    live = slots < answer_count[0]
    wanted = my_start + slots
    mine = wanted[:, None] == ids
    mine = jnp.sum(jnp.where(mine[None, None], table, 0.0), axis=3)
    log_total = jnp.log(mine[0])
    logprob = mine[2] - log_total
    divergence = mine[1, :LAYERS] / mine[0, LAYERS:] - log_total[LAYERS:] + log_total[:LAYERS]
    logprob = jnp.where(live[None], logprob, 0.0)[:, None, :]
    divergence = jnp.where(live[None], divergence, 0.0)[:, None, :]
    return (logprob, divergence)


def solution(mesh):
    split = Mesh(mesh.devices.reshape(4, 2, 2, 4, 4), ("zq", "zp", "c", "y", "x"))
    return jax.shard_map(
        body,
        mesh=split,
        in_specs=(
            P(None, SEQ, VOCAB),
            P(SEQ, VOCAB),
            P(None, VOCAB, SEQ),
            P(None, SEQ),
            P(SEQ),
            P(VOCAB, SEQ),
            P(SEQ, None),
            P(SEQ),
            P(SEQ, None),
        ),
        out_specs=(P(None, SEQ, None), P(None, SEQ, None)),
        check_vma=False,
    )
```

```python
import functools

import jax
import jax.numpy as jnp
from jax import lax
from jax.experimental import pallas as pl
from jax.experimental.pallas import tpu as pltpu
from jax.sharding import Mesh
from jax.sharding import PartitionSpec as P


D = 6144
LAYERS = 3
CAP = 32
ROWS = 256
Z = ("zq", "zp")
SEQ = ("zq", "zp", "c")
VOCAB = ("y", "x")
F32 = jnp.float32
BF16 = jnp.bfloat16
NT = (((1,), (1,)), ((), ()))
TN = (((0,), (0,)), ((), ()))
INFO = 96
OFFSETS = (0, -2, 2, -1, 1, -3, 3, -4)
SHIFT = 16.0
SCALE = 262144.0
LARGE = 16.0


def dot(a, b):
    return jnp.dot(a, b, preferred_element_type=F32)


def exchange(value, axes):
    return lax.all_to_all(value, axes, split_axis=0, concat_axis=0, tiled=True)


def shifted(value, by):
    return lax.ppermute(value, Z, [(j, (j + by) % 8) for j in range(8)])


def swap_cores(value):
    return lax.ppermute(value, "c", [(0, 1), (1, 0)])


def whole(shape, dtype):
    return pltpu.VMEM(shape, dtype)


def far(shape, dtype):
    return pltpu.HBM(shape, dtype)


def near(value):
    return pltpu.with_memory_space_constraint(value, pltpu.VMEM)


def held(value):
    return pltpu.with_memory_space_constraint(value, pltpu.HBM)


SCALARS = pl.BlockSpec(memory_space=pltpu.SMEM)
VECTORS = pl.BlockSpec(memory_space=pltpu.VMEM)
LIMIT = pltpu.CompilerParams(vmem_limit_bytes=24 * 1024 * 1024)


def pick_kernel(picks, count, targets, probe, final_far, out, last, rows, final, arrived):
    fetch = pltpu.make_async_copy(final_far, final, arrived)
    fetch.start()
    sub = lax.broadcasted_iota(jnp.int32, (16, out.shape[1]), 0)

    def take(layer, k):
        pick = jnp.clip(picks[0, k], 0, final.shape[0] - 1)
        within = lax.rem(pick, 16)
        group = pl.ds(pl.multiple_of(pick - within, 16), 16)
        block = probe[layer, group, :] if layer < LAYERS else final[group, :]
        row = jnp.sum(jnp.where(sub == within, block.astype(F32), 0.0), axis=0, keepdims=True)
        rows[layer * CAP + k : layer * CAP + k + 1, :] = row

    for k in range(CAP):
        for layer in range(LAYERS):
            take(layer, k)
    fetch.wait()
    for k in range(CAP):
        take(LAYERS, k)
    out[0:INFO] = rows[0:INFO].astype(BF16)
    last[...] = rows[INFO : INFO + CAP].astype(BF16)
    out[INFO : INFO + 8] = jnp.zeros((8, out.shape[1]), BF16)
    line = lax.broadcasted_iota(jnp.int32, (8, CAP), 0)
    wanted = jnp.broadcast_to(targets[...], (8, CAP))
    value = jnp.where(line == 0, wanted >> 8, jnp.where(line == 1, wanted & 255, jnp.where(line == 2, count[0], 0)))
    out[INFO : INFO + 8, 0:CAP] = value.astype(F32).astype(BF16)


def translate_kernel(flags, *refs):
    own, other = refs[:8], refs[8:16]
    final, translator, out, info = refs[16:]
    low_core = flags[0] == 0
    keep = flags[1].astype(F32)
    chips = [lax.rem(flags[4] + offset + 8, 8) for offset in OFFSETS]
    lane = lax.broadcasted_iota(jnp.int32, (CAP, ROWS), 1).astype(F32)
    slot = lax.broadcasted_iota(jnp.int32, (CAP, ROWS), 0).astype(F32)
    counts_own = [ref[INFO + 2 : INFO + 3, 0:1].astype(F32) for ref in own]
    counts_other = [ref[INFO + 2 : INFO + 3, 0:1].astype(F32) for ref in other]
    start = jnp.zeros((1, 1), F32)
    count = jnp.zeros((1, 1), F32)
    for k in range(8):
        for seq, value in ((2 * chips[k] + flags[0], counts_own[k]), (2 * chips[k] + 1 - flags[0], counts_other[k])):
            start = start + jnp.where(seq < flags[5], value, 0.0)
            count = count + jnp.where(seq == flags[5], value, 0.0)
    pick_final = jnp.where((lane == start + slot) & (slot < count), 1.0, 0.0).astype(BF16)
    pick_own, pick_other = [], []
    for k in range(8):
        base = jnp.zeros((1, 1), F32)
        for j in range(8):
            if j != k:
                base = base + jnp.where(chips[j] < chips[k], counts_own[j] + counts_other[j], 0.0)
        start_own = base + jnp.where(low_core, 0.0, counts_other[k])
        start_other = base + jnp.where(low_core, counts_own[k], 0.0)
        hit_own = (lane == start_own + slot) & (slot < counts_own[k])
        hit_other = (lane == start_other + slot) & (slot < counts_other[k])
        pick_own.append(jnp.where(hit_own, 1.0, 0.0).astype(BF16))
        pick_other.append(jnp.where(hit_other, 1.0, 0.0).astype(BF16))
        a = own[k][INFO : INFO + 8, 0:128].astype(F32)
        b = other[k][INFO : INFO + 8, 0:128].astype(F32)
        info[2 * chips[k]] = jnp.where(low_core, a, b)
        info[2 * chips[k] + 1] = jnp.where(low_core, b, a)
    pick_own = jnp.concatenate(pick_own, axis=0)
    pick_other = jnp.concatenate(pick_other, axis=0)
    for layer in range(LAYERS):
        low = layer * CAP
        a = jnp.concatenate([ref[low : low + CAP, :] for ref in own], axis=0)
        b = jnp.concatenate([ref[low : low + CAP, :] for ref in other], axis=0)
        rows = lax.dot_general(pick_own, a, TN, preferred_element_type=F32)
        rows = rows + lax.dot_general(pick_other, b, TN, preferred_element_type=F32)
        part = rows * keep + dot(rows.astype(BF16), translator[layer])
        out[:, layer] = part.astype(BF16).reshape(16, 16, -1)
    rows = lax.dot_general(pick_final, final[...], TN, preferred_element_type=F32)
    out[:, LAYERS] = rows.astype(BF16).reshape(16, 16, -1)


def high_low(value):
    high = value.astype(BF16).astype(F32)
    row = lax.broadcasted_iota(jnp.int32, value.shape, 0)
    return jnp.where(row == 0, high, jnp.where(row == 1, value - high, 0.0))


def scale_kernel(parts, bias, gain, y_out):
    x = parts[0].astype(F32)
    for k in range(1, 16):
        x = x + parts[k].astype(F32)
    x = x + bias[...]
    y = (x * gain[...]).astype(BF16)
    square = x * x
    square = jnp.concatenate([square] * 4, axis=0)
    ones = jnp.ones((8, x.shape[1]), F32)
    squares = lax.dot_general(ones, square, NT, precision=lax.Precision.HIGHEST, preferred_element_type=F32)
    squares = high_low(squares)
    for k in range(32):
        y_out[k, 0:64] = y
        y_out[k, 64:72] = jnp.zeros((8, x.shape[1]), BF16)
        y_out[k, 64:72, 0:256] = squares.astype(BF16)


def squares_of(y, chunk):
    lane = lax.broadcasted_iota(jnp.int32, (8, 256), 1)
    square = jnp.zeros((8, 256), F32)
    for j in range(4):
        total = jnp.zeros((1, 256), F32)
        for half in range(2):
            both = y[16 * half + 4 * chunk + j, 64:72, 0:256].astype(F32)
            total = total + both[0:1] + both[1:2]
        square = jnp.where(lane // 64 == j, jnp.broadcast_to(total, (8, 256)), square)
    return square


def own_kernel(flags, y, u_near, u_far, out):
    pair = flags[2]
    a = y[pl.ds(16 * pair, 16), 0:64, :].reshape(1024, -1)
    b = y[pl.ds(16 * (1 - pair), 16), 0:64, :].reshape(1024, -1)
    part = lax.dot_general(a, u_near[...], NT, preferred_element_type=F32)
    part = part + lax.dot_general(b, u_far[...], NT, preferred_element_type=F32)
    out[:, 0:256, :] = part.reshape(4, 256, -1)
    for k in range(4):
        out[k, 256:264, 0:256] = squares_of(y, k)


def chunk_kernel(step, flags, own_part, y_other, u_near, u_far, out):
    pair = flags[2]
    chunk = (flags[3] + step) % 4
    a = y_other[pl.ds(16 * pair + 4 * chunk, 4), 0:64, :].reshape(256, -1)
    b = y_other[pl.ds(16 * (1 - pair) + 4 * chunk, 4), 0:64, :].reshape(256, -1)
    part = lax.dot_general(a, u_near[...], NT, preferred_element_type=F32)
    part = part + lax.dot_general(b, u_far[...], NT, preferred_element_type=F32)
    out[0:256, :] = (own_part[chunk, 0:256, :] + part) * (1.0 / SHIFT)
    out[256:264, :] = jnp.zeros((8, out.shape[1]), F32)
    square = own_part[chunk, 256:264, 0:256] + squares_of(y_other, chunk)
    row = lax.broadcasted_iota(jnp.int32, square.shape, 0)
    large = square >= LARGE
    value = jnp.where(row < 2, jnp.where(large, square * (1.0 / SCALE), 0.0), jnp.where(large, 0.0, square))
    high = value.astype(BF16).astype(F32)
    value = jnp.where(row % 2 == 0, high, value - high)
    out[256:264, 0:256] = jnp.where(row < 4, value, 0.0)


def stats_kernel(summed, target, out):
    rows = summed[256:264, 0:256]
    square = (rows[0:1] + rows[1:2]) * SCALE + rows[2:3] + rows[3:4]
    factor = SHIFT * lax.rsqrt(square * (1.0 / D) + 1e-05)
    factor = jnp.broadcast_to(factor, (128, 256)).T[:, 0:1]
    logits = summed[0:256] * factor
    width = logits.shape[1]
    expz = jnp.exp(logits)
    total = jnp.sum(expz, axis=1, keepdims=True)
    ids = lax.broadcasted_iota(jnp.int32, logits.shape, 1)
    picked = jnp.sum(jnp.where(ids == target[...], logits, 0.0), axis=1, keepdims=True)
    four = logits.reshape(4, 4, 16, width)
    last = expz.reshape(4, 4, 16, width)[:, 3:]
    cross = jnp.sum(last * (four[:, 3:] - four), axis=3, keepdims=True).reshape(256, 1)
    lane = lax.broadcasted_iota(jnp.int32, (128, 128), 1)
    table = jnp.zeros((128, 128), F32)
    for h in range(2):
        for k, value in enumerate((total, cross, picked)):
            table = jnp.where(lane == 3 * h + k, value[128 * h : 128 * h + 128], table)
    rows = table.T[:8]
    for k in range(64):
        out[k] = rows


def body(
    probe_states,
    final_states,
    translator,
    translator_bias,
    norm_gain,
    unembed,
    answer_rows,
    answer_count,
    targets,
):
    zq = lax.axis_index("zq")
    c = lax.axis_index("c")
    quarter = 2 * lax.axis_index("zp") + c
    v = lax.axis_index(VOCAB)
    seq = 4 * zq + quarter
    width = probe_states.shape[2]
    part = unembed.shape[0] // 4

    local, last = pl.pallas_call(
        pick_kernel,
        out_shape=(whole((INFO + 8, width), BF16), whole((CAP, width), BF16)),
        in_specs=[SCALARS] * 2 + [VECTORS] * 2 + [pl.BlockSpec(memory_space=pltpu.HBM)],
        out_specs=(VECTORS, VECTORS),
        scratch_shapes=[
            pltpu.VMEM((INFO + CAP, width), F32),
            pltpu.VMEM(final_states.shape, BF16),
            pltpu.SemaphoreType.DMA(()),
        ],
        compiler_params=LIMIT,
        name="pick",
    )(answer_rows, answer_count, held(targets), near(probe_states), held(final_states))
    back2, fore2, back1, fore1 = [shifted(local, by) for by in (2, -2, 1, -1)]
    own = [local, back2, fore2, back1, fore1]
    other = [swap_cores(chunk) for chunk in own[1:]]
    other = [swap_cores(local)] + other
    turned = [(a * 16 + b, b * 16 + a) for a in range(16) for b in range(16)]
    last = lax.ppermute(last, (*SEQ, *VOCAB), turned)
    third = [shifted(back2, 1), shifted(fore2, -1), shifted(back2, 2)]
    own += third
    other += [swap_cores(chunk) for chunk in third]

    flags = jnp.stack([c, (seq == v).astype(jnp.int32), quarter // 2, zq, seq // 2, v])
    parts, every_info = pl.pallas_call(
        translate_kernel,
        out_shape=(far((16, 4, 16, width), BF16), far((16, 8, 128), F32)),
        in_specs=[SCALARS] + [VECTORS] * 18,
        out_specs=(VECTORS, VECTORS),
        compiler_params=LIMIT,
        name="translate",
    )(flags, *[near(chunk) for chunk in own + other], near(last), near(translator))
    arrived = exchange(parts.reshape(16, 64, width), VOCAB)
    fours = unembed.reshape(4, part, width)
    quarters = []
    for k in range(4):
        block = lax.dynamic_index_in_dim(fours, quarter ^ k, 0, keepdims=False)
        if k:
            block = lax.ppermute(block, ("zp", "c"), [(j, j ^ k) for j in range(4)])
        quarters.append(block)

    bias = jnp.concatenate([translator_bias, jnp.zeros((1, width), F32)], axis=0)
    bias = jnp.repeat(bias, 16, axis=0)
    y_copies = pl.pallas_call(
        scale_kernel,
        out_shape=whole((32, 72, width), BF16),
        in_specs=[VECTORS] * 3,
        out_specs=VECTORS,
        compiler_params=LIMIT,
        name="scale",
    )(near(arrived), bias, norm_gain[None, :])
    y_own = exchange(y_copies, ("zp", *VOCAB))
    y_other = swap_cores(y_own)

    quarters = [near(block) for block in quarters]
    y_own, y_other = near(y_own), near(y_other)
    own_part = pl.pallas_call(
        own_kernel,
        out_shape=whole((4, 264, part), F32),
        in_specs=[SCALARS] + [VECTORS] * 3,
        out_specs=VECTORS,
        compiler_params=LIMIT,
        name="own_logits",
    )(flags, y_own, quarters[0], quarters[2])
    chunks = []
    for k in (2, 1, 3, 0):
        chunk = pl.pallas_call(
            functools.partial(chunk_kernel, k),
            out_shape=whole((264, part), F32),
            in_specs=[SCALARS] + [VECTORS] * 4,
            out_specs=VECTORS,
            compiler_params=LIMIT,
        )(flags, near(own_part), y_other, quarters[1], quarters[3])
        if k:
            chunk = chunk.astype(jnp.float16)
            chunk = lax.ppermute(chunk, "zq", [(j, (j + k) % 4) for j in range(4)])
        else:
            every_info, chunk = lax.optimization_barrier((every_info, chunk))
        chunks.append(chunk)
    summed = chunks[3]
    for chunk in chunks[:3]:
        summed = summed + chunk.astype(F32)

    every_info = every_info[:, :3, :CAP].astype(jnp.int32)
    counts = every_info[:, 2, 0]
    all_targets = every_info[:, 0] * 256 + every_info[:, 1]
    order = jnp.arange(16, dtype=jnp.int32)
    starts = jnp.sum(jnp.where(order[None, :] < order[:, None], counts[None, :], 0), axis=1)
    slots = jnp.arange(CAP, dtype=jnp.int32)
    place = jnp.where(slots[None, :] < counts[:, None], starts[:, None] + slots[None, :], -1)
    row_ids = zq * 64 + jnp.arange(64, dtype=jnp.int32)
    hit = place[None] == row_ids[:, None, None]
    row_targets = jnp.sum(jnp.where(hit, all_targets[None], 0), axis=(1, 2))
    local_targets = row_targets - (v * 4 + quarter) * part
    item_targets = jnp.broadcast_to(local_targets.reshape(4, 1, 16), (4, 4, 16)).reshape(256, 1)
    stats = pl.pallas_call(
        stats_kernel,
        out_shape=far((64, 8, 128), F32),
        in_specs=[VECTORS] * 2,
        out_specs=VECTORS,
        compiler_params=LIMIT,
        name="stats",
    )(near(summed), item_targets)
    sums = jnp.sum(exchange(stats, ("zp", "c", *VOCAB)), axis=0)
    every = [sums]
    for k in (1, 2, 3):
        every.append(lax.ppermute(sums, "zq", [(j, (j + k) % 4) for j in range(4)]))
    every = jnp.stack(every)

    table = every[:, :6].reshape(4, 2, 3, 2, 4, 16).transpose(2, 4, 0, 1, 3, 5).reshape(3, 4, 1, ROWS)
    chunk = (zq - jnp.arange(4, dtype=jnp.int32)) % 4
    ids = (chunk[:, None] * 64 + jnp.arange(64, dtype=jnp.int32)[None, :]).reshape(1, ROWS)
    my_start = jnp.sum(jnp.where(order == seq, starts, 0))
    live = slots < answer_count[0]
    wanted = my_start + slots
    mine = wanted[:, None] == ids
    mine = jnp.sum(jnp.where(mine[None, None], table, 0.0), axis=3)
    log_total = jnp.log(mine[0])
    logprob = mine[2] - log_total
    divergence = mine[1, :LAYERS] / mine[0, LAYERS:] - log_total[LAYERS:] + log_total[:LAYERS]
    logprob = jnp.where(live[None], logprob, 0.0)[:, None, :]
    divergence = jnp.where(live[None], divergence, 0.0)[:, None, :]
    return (logprob, divergence)


def solution(mesh):
    split = Mesh(mesh.devices.reshape(4, 2, 2, 4, 4), ("zq", "zp", "c", "y", "x"))
    return jax.shard_map(
        body,
        mesh=split,
        in_specs=(
            P(None, SEQ, VOCAB),
            P(SEQ, VOCAB),
            P(None, VOCAB, SEQ),
            P(None, SEQ),
            P(SEQ),
            P(VOCAB, SEQ),
            P(SEQ, None),
            P(SEQ),
            P(SEQ, None),
        ),
        out_specs=(P(None, SEQ, None), P(None, SEQ, None)),
        check_vma=False,
    )
```

```python
import functools

import jax
import jax.numpy as jnp
from jax import lax
from jax.experimental import pallas as pl
from jax.experimental.pallas import tpu as pltpu
from jax.sharding import Mesh
from jax.sharding import PartitionSpec as P


D = 6144
LAYERS = 3
CAP = 32
ROWS = 256
Z = ("zq", "zp")
SEQ = ("zq", "zp", "c")
VOCAB = ("y", "x")
F32 = jnp.float32
BF16 = jnp.bfloat16
NT = (((1,), (1,)), ((), ()))
TN = (((0,), (0,)), ((), ()))
INFO = 128
OFFSETS = (0, -2, 2, -1, 1, -3, 3, -4)
SHIFT = 16.0
SCALE = 262144.0
LARGE = 16.0


def dot(a, b):
    return jnp.dot(a, b, preferred_element_type=F32)


def exchange(value, axes):
    return lax.all_to_all(value, axes, split_axis=0, concat_axis=0, tiled=True)


def shifted(value, by):
    return lax.ppermute(value, Z, [(j, (j + by) % 8) for j in range(8)])


def swap_cores(value):
    return lax.ppermute(value, "c", [(0, 1), (1, 0)])


def whole(shape, dtype):
    return pltpu.VMEM(shape, dtype)


def far(shape, dtype):
    return pltpu.HBM(shape, dtype)


def near(value):
    return pltpu.with_memory_space_constraint(value, pltpu.VMEM)


def held(value):
    return pltpu.with_memory_space_constraint(value, pltpu.HBM)


SCALARS = pl.BlockSpec(memory_space=pltpu.SMEM)
VECTORS = pl.BlockSpec(memory_space=pltpu.VMEM)
LIMIT = pltpu.CompilerParams(vmem_limit_bytes=24 * 1024 * 1024)


def pick_kernel(picks, count, targets, probe_far, final_far, out, rows, probe, final, arrived):
    copies = [pltpu.make_async_copy(probe_far.at[k], probe.at[k], arrived.at[k]) for k in range(LAYERS)]
    copies.append(pltpu.make_async_copy(final_far, final, arrived.at[LAYERS]))
    for copy in copies:
        copy.start()
    sub = lax.broadcasted_iota(jnp.int32, (16, out.shape[1]), 0)
    for layer in range(LAYERS + 1):
        copies[layer].wait()
        for k in range(CAP):
            pick = jnp.clip(picks[0, k], 0, final.shape[0] - 1)
            within = lax.rem(pick, 16)
            group = pl.ds(pl.multiple_of(pick - within, 16), 16)
            block = probe[layer, group, :] if layer < LAYERS else final[group, :]
            row = jnp.sum(jnp.where(sub == within, block.astype(F32), 0.0), axis=0, keepdims=True)
            rows[layer * CAP + k : layer * CAP + k + 1, :] = row
    out[0:INFO] = rows[...].astype(BF16)
    out[INFO : INFO + 8] = jnp.zeros((8, out.shape[1]), BF16)
    line = lax.broadcasted_iota(jnp.int32, (8, CAP), 0)
    wanted = jnp.broadcast_to(targets[...], (8, CAP))
    value = jnp.where(line == 0, wanted >> 8, jnp.where(line == 1, wanted & 255, jnp.where(line == 2, count[0], 0)))
    out[INFO : INFO + 8, 0:CAP] = value.astype(F32).astype(BF16)


def translate_kernel(flags, *refs):
    own, other = refs[:8], refs[8:16]
    translator, out, info = refs[16:]
    low_core = flags[0] == 0
    keep = flags[1].astype(F32)
    chips = [lax.rem(flags[4] + offset + 8, 8) for offset in OFFSETS]
    lane = lax.broadcasted_iota(jnp.int32, (CAP, ROWS), 1).astype(F32)
    slot = lax.broadcasted_iota(jnp.int32, (CAP, ROWS), 0).astype(F32)
    counts_own = [ref[INFO + 2 : INFO + 3, 0:1].astype(F32) for ref in own]
    counts_other = [ref[INFO + 2 : INFO + 3, 0:1].astype(F32) for ref in other]
    pick_own, pick_other = [], []
    for k in range(8):
        base = jnp.zeros((1, 1), F32)
        for j in range(8):
            if j != k:
                base = base + jnp.where(chips[j] < chips[k], counts_own[j] + counts_other[j], 0.0)
        start_own = base + jnp.where(low_core, 0.0, counts_other[k])
        start_other = base + jnp.where(low_core, counts_own[k], 0.0)
        hit_own = (lane == start_own + slot) & (slot < counts_own[k])
        hit_other = (lane == start_other + slot) & (slot < counts_other[k])
        pick_own.append(jnp.where(hit_own, 1.0, 0.0).astype(BF16))
        pick_other.append(jnp.where(hit_other, 1.0, 0.0).astype(BF16))
        a = own[k][INFO : INFO + 8, 0:128].astype(F32)
        b = other[k][INFO : INFO + 8, 0:128].astype(F32)
        info[2 * chips[k]] = jnp.where(low_core, a, b)
        info[2 * chips[k] + 1] = jnp.where(low_core, b, a)
    pick_own = jnp.concatenate(pick_own, axis=0)
    pick_other = jnp.concatenate(pick_other, axis=0)
    for layer in range(LAYERS + 1):
        low = layer * CAP
        a = jnp.concatenate([ref[low : low + CAP, :] for ref in own], axis=0)
        b = jnp.concatenate([ref[low : low + CAP, :] for ref in other], axis=0)
        rows = lax.dot_general(pick_own, a, TN, preferred_element_type=F32)
        rows = rows + lax.dot_general(pick_other, b, TN, preferred_element_type=F32)
        part = rows * keep
        if layer < LAYERS:
            part = part + dot(rows.astype(BF16), translator[layer])
        out[:, layer] = part.astype(BF16).reshape(16, 16, -1)


def high_low(value):
    high = value.astype(BF16).astype(F32)
    row = lax.broadcasted_iota(jnp.int32, value.shape, 0)
    return jnp.where(row == 0, high, jnp.where(row == 1, value - high, 0.0))


def scale_kernel(parts, bias, gain, y_out):
    x = parts[0].astype(F32)
    for k in range(1, 16):
        x = x + parts[k].astype(F32)
    x = x + bias[...]
    y = (x * gain[...]).astype(BF16)
    square = x * x
    square = jnp.concatenate([square] * 4, axis=0)
    ones = jnp.ones((8, x.shape[1]), F32)
    squares = lax.dot_general(ones, square, NT, precision=lax.Precision.HIGHEST, preferred_element_type=F32)
    squares = high_low(squares)
    for k in range(32):
        y_out[k, 0:64] = y
        y_out[k, 64:72] = jnp.zeros((8, x.shape[1]), BF16)
        y_out[k, 64:72, 0:256] = squares.astype(BF16)


def squares_of(y, chunk):
    lane = lax.broadcasted_iota(jnp.int32, (8, 256), 1)
    square = jnp.zeros((8, 256), F32)
    for j in range(4):
        total = jnp.zeros((1, 256), F32)
        for half in range(2):
            both = y[16 * half + 4 * chunk + j, 64:72, 0:256].astype(F32)
            total = total + both[0:1] + both[1:2]
        square = jnp.where(lane // 64 == j, jnp.broadcast_to(total, (8, 256)), square)
    return square


def own_kernel(flags, y, u_near, u_far, out):
    pair = flags[2]
    a = y[pl.ds(16 * pair, 16), 0:64, :].reshape(1024, -1)
    b = y[pl.ds(16 * (1 - pair), 16), 0:64, :].reshape(1024, -1)
    part = lax.dot_general(a, u_near[...], NT, preferred_element_type=F32)
    part = part + lax.dot_general(b, u_far[...], NT, preferred_element_type=F32)
    out[:, 0:256, :] = part.reshape(4, 256, -1)
    for k in range(4):
        out[k, 256:264, 0:256] = squares_of(y, k)


def chunk_kernel(step, flags, own_part, y_other, u_near, u_far, out):
    pair = flags[2]
    chunk = (flags[3] + step) % 4
    a = y_other[pl.ds(16 * pair + 4 * chunk, 4), 0:64, :].reshape(256, -1)
    b = y_other[pl.ds(16 * (1 - pair) + 4 * chunk, 4), 0:64, :].reshape(256, -1)
    part = lax.dot_general(a, u_near[...], NT, preferred_element_type=F32)
    part = part + lax.dot_general(b, u_far[...], NT, preferred_element_type=F32)
    out[0:256, :] = (own_part[chunk, 0:256, :] + part) * (1.0 / SHIFT)
    out[256:264, :] = jnp.zeros((8, out.shape[1]), F32)
    square = own_part[chunk, 256:264, 0:256] + squares_of(y_other, chunk)
    row = lax.broadcasted_iota(jnp.int32, square.shape, 0)
    large = square >= LARGE
    value = jnp.where(row < 2, jnp.where(large, square * (1.0 / SCALE), 0.0), jnp.where(large, 0.0, square))
    high = value.astype(BF16).astype(F32)
    value = jnp.where(row % 2 == 0, high, value - high)
    out[256:264, 0:256] = jnp.where(row < 4, value, 0.0)


def stats_kernel(summed, target, out):
    rows = summed[256:264, 0:256]
    square = (rows[0:1] + rows[1:2]) * SCALE + rows[2:3] + rows[3:4]
    factor = SHIFT * lax.rsqrt(square * (1.0 / D) + 1e-05)
    factor = jnp.broadcast_to(factor, (128, 256)).T[:, 0:1]
    logits = summed[0:256] * factor
    width = logits.shape[1]
    expz = jnp.exp(logits)
    total = jnp.sum(expz, axis=1, keepdims=True)
    ids = lax.broadcasted_iota(jnp.int32, logits.shape, 1)
    picked = jnp.sum(jnp.where(ids == target[...], logits, 0.0), axis=1, keepdims=True)
    four = logits.reshape(4, 4, 16, width)
    last = expz.reshape(4, 4, 16, width)[:, 3:]
    cross = jnp.sum(last * (four[:, 3:] - four), axis=3, keepdims=True).reshape(256, 1)
    lane = lax.broadcasted_iota(jnp.int32, (128, 128), 1)
    table = jnp.zeros((128, 128), F32)
    for h in range(2):
        for k, value in enumerate((total, cross, picked)):
            table = jnp.where(lane == 3 * h + k, value[128 * h : 128 * h + 128], table)
    out[...] = table.T[:8]


def body(
    probe_states,
    final_states,
    translator,
    translator_bias,
    norm_gain,
    unembed,
    answer_rows,
    answer_count,
    targets,
):
    zq = lax.axis_index("zq")
    c = lax.axis_index("c")
    quarter = 2 * lax.axis_index("zp") + c
    v = lax.axis_index(VOCAB)
    seq = 4 * zq + quarter
    width = probe_states.shape[2]
    part = unembed.shape[0] // 4

    local = pl.pallas_call(
        pick_kernel,
        out_shape=whole((INFO + 8, width), BF16),
        in_specs=[SCALARS] * 2 + [VECTORS] + [pl.BlockSpec(memory_space=pltpu.HBM)] * 2,
        out_specs=VECTORS,
        scratch_shapes=[
            pltpu.VMEM((INFO, width), F32),
            pltpu.VMEM(probe_states.shape, BF16),
            pltpu.VMEM(final_states.shape, BF16),
            pltpu.SemaphoreType.DMA((LAYERS + 1,)),
        ],
        compiler_params=LIMIT,
        name="pick",
    )(answer_rows, answer_count, held(targets), held(probe_states), held(final_states))
    back2, fore2, back1, fore1 = [shifted(local, by) for by in (2, -2, 1, -1)]
    own = [local, back2, fore2, back1, fore1]
    other = [swap_cores(chunk) for chunk in own]
    third = [shifted(back2, 1), shifted(fore2, -1), shifted(back2, 2)]
    own += third
    other += [swap_cores(chunk) for chunk in third]

    flags = jnp.stack([c, (seq == v).astype(jnp.int32), quarter // 2, zq, seq // 2])
    parts, every_info = pl.pallas_call(
        translate_kernel,
        out_shape=(far((16, 4, 16, width), BF16), far((16, 8, 128), F32)),
        in_specs=[SCALARS] + [VECTORS] * 17,
        out_specs=(VECTORS, VECTORS),
        compiler_params=LIMIT,
        name="translate",
    )(flags, *[near(chunk) for chunk in own + other], near(translator))
    arrived = exchange(parts.reshape(16, 64, width), VOCAB)
    fours = unembed.reshape(4, part, width)
    quarters = []
    for k in range(4):
        block = lax.dynamic_index_in_dim(fours, quarter ^ k, 0, keepdims=False)
        if k:
            block = lax.ppermute(block, ("zp", "c"), [(j, j ^ k) for j in range(4)])
        quarters.append(block)

    bias = jnp.concatenate([translator_bias, jnp.zeros((1, width), F32)], axis=0)
    bias = jnp.repeat(bias, 16, axis=0)
    y_copies = pl.pallas_call(
        scale_kernel,
        out_shape=whole((32, 72, width), BF16),
        in_specs=[VECTORS] * 3,
        out_specs=VECTORS,
        compiler_params=LIMIT,
        name="scale",
    )(near(arrived), bias, norm_gain[None, :])
    y_own = exchange(y_copies, ("zp", *VOCAB))
    y_other = swap_cores(y_own)

    quarters = [near(block) for block in quarters]
    y_own, y_other = held(y_own), near(y_other)
    own_part = pl.pallas_call(
        own_kernel,
        out_shape=whole((4, 264, part), F32),
        in_specs=[SCALARS] + [VECTORS] * 3,
        out_specs=VECTORS,
        compiler_params=LIMIT,
        name="own_logits",
    )(flags, y_own, quarters[0], quarters[2])
    chunks = []
    for k in (2, 1, 3, 0):
        chunk = pl.pallas_call(
            functools.partial(chunk_kernel, k),
            out_shape=whole((264, part), F32),
            in_specs=[SCALARS] + [VECTORS] * 4,
            out_specs=VECTORS,
            compiler_params=LIMIT,
        )(flags, near(own_part), y_other, quarters[1], quarters[3])
        if k:
            chunk = chunk.astype(jnp.float16)
            chunk = lax.ppermute(chunk, "zq", [(j, (j + k) % 4) for j in range(4)])
        else:
            every_info, chunk = lax.optimization_barrier((every_info, chunk))
        chunks.append(chunk)
    summed = chunks[3]
    for chunk in chunks[:3]:
        summed = summed + chunk.astype(F32)

    every_info = every_info[:, :3, :CAP].astype(jnp.int32)
    counts = every_info[:, 2, 0]
    all_targets = every_info[:, 0] * 256 + every_info[:, 1]
    order = jnp.arange(16, dtype=jnp.int32)
    starts = jnp.sum(jnp.where(order[None, :] < order[:, None], counts[None, :], 0), axis=1)
    slots = jnp.arange(CAP, dtype=jnp.int32)
    place = jnp.where(slots[None, :] < counts[:, None], starts[:, None] + slots[None, :], -1)
    row_ids = zq * 64 + jnp.arange(64, dtype=jnp.int32)
    hit = place[None] == row_ids[:, None, None]
    row_targets = jnp.sum(jnp.where(hit, all_targets[None], 0), axis=(1, 2))
    local_targets = row_targets - (v * 4 + quarter) * part
    item_targets = jnp.broadcast_to(local_targets.reshape(4, 1, 16), (4, 4, 16)).reshape(256, 1)
    stats = pl.pallas_call(
        stats_kernel,
        out_shape=whole((8, 128), F32),
        in_specs=[VECTORS] * 2,
        out_specs=VECTORS,
        compiler_params=LIMIT,
        name="stats",
    )(near(summed), item_targets)
    stats = stats + swap_cores(stats)
    sums = jnp.sum(exchange(jnp.broadcast_to(stats[None], (32, 8, 128)), ("zp", *VOCAB)), axis=0)
    every = [sums]
    for k in (1, 2, 3):
        every.append(lax.ppermute(sums, "zq", [(j, (j + k) % 4) for j in range(4)]))
    every = jnp.stack(every)

    table = every[:, :6].reshape(4, 2, 3, 2, 4, 16).transpose(2, 4, 0, 1, 3, 5).reshape(3, 4, 1, ROWS)
    chunk = (zq - jnp.arange(4, dtype=jnp.int32)) % 4
    ids = (chunk[:, None] * 64 + jnp.arange(64, dtype=jnp.int32)[None, :]).reshape(1, ROWS)
    my_start = jnp.sum(jnp.where(order == seq, starts, 0))
    live = slots < answer_count[0]
    wanted = my_start + slots
    mine = wanted[:, None] == ids
    mine = jnp.sum(jnp.where(mine[None, None], table, 0.0), axis=3)
    log_total = jnp.log(mine[0])
    logprob = mine[2] - log_total
    divergence = mine[1, :LAYERS] / mine[0, LAYERS:] - log_total[LAYERS:] + log_total[:LAYERS]
    logprob = jnp.where(live[None], logprob, 0.0)[:, None, :]
    divergence = jnp.where(live[None], divergence, 0.0)[:, None, :]
    return (logprob, divergence)


def solution(mesh):
    split = Mesh(mesh.devices.reshape(4, 2, 2, 4, 4), ("zq", "zp", "c", "y", "x"))
    return jax.shard_map(
        body,
        mesh=split,
        in_specs=(
            P(None, SEQ, VOCAB),
            P(SEQ, VOCAB),
            P(None, VOCAB, SEQ),
            P(None, SEQ),
            P(SEQ),
            P(VOCAB, SEQ),
            P(SEQ, None),
            P(SEQ),
            P(SEQ, None),
        ),
        out_specs=(P(None, SEQ, None), P(None, SEQ, None)),
        check_vma=False,
    )
```
